32 devices in a mesh: row: 4 (over y, x), col: 8 (over z, core).
Axes of the slice: x: 2, y: 2, z: 4, core: 2. Of those that a mesh axis runs over, the one named last changes fastest.
Arguments:
- values: bfloat16 [4096, 4096], P('row', 'col'), may hold values from 0.0001296997 to 0.12988281
- tile_mask: int32 [32, 32], P('row', 'col'), may hold values 0 or 1
- keep_mask: int32 [32, 32], P('row', 'col'), may hold values 0 or 1
- thr_index: int32 [4096], P('col'), may hold values from 0 to 9
Outputs:
- expanded: bfloat16 [4096, 4096], P('row', 'col')
The draws below stay inside these ranges and needn't reach their ends.
All inputs are finite; a program needn't handle non-finite values. No bound on the sum of `tile_mask` or of `keep_mask` on one device may be relied on, other than what follows from the above.
Results may differ from the reference program's by a relative error of at most 0.0004.
Values may be sent and summed in bfloat16 or wider, within the bound.
A program may use at most 64 MiB of HBM per device.

```python
import math
import jax
import jax.numpy as jnp

TB = 128
NT = 32
ORDER = 4096


def touch_ends(values, stream_key, smallest, largest):
    spot = [jax.random.randint(jax.random.fold_in(stream_key, axis), (), 0, length) for axis, length in enumerate(values.shape)]
    longest = values.shape.index(max(values.shape))
    neighbour = spot[:longest] + [(spot[longest] + 1) % values.shape[longest]] + spot[longest + 1:]
    return values.at[tuple(spot)].set(smallest).at[tuple(neighbour)].set(largest)


def levels(stream_key, extent, shards, least, largest):
    level = 1.0
    for dim, shards_of in shards:
        draws = jax.random.uniform(jax.random.fold_in(jax.random.fold_in(stream_key, 6), dim), (shards_of,), jnp.float32, least / len(shards), largest / len(shards))
        level = level * jnp.repeat(jnp.exp(draws), extent[dim] // shards_of).reshape((-1,) + (1,) * (len(extent) - 1 - dim))
    return level


def setup_inputs(seed: int = 0) -> dict:
    seeds = jax.random.split(jax.random.key(seed), 5)
    values = jnp.clip(jnp.exp(math.log(0.12988281) - 6.909166 * jax.random.uniform(seeds[0], (ORDER, ORDER), jnp.float32) ** levels(seeds[0], (ORDER, ORDER), ((0, 4), (1, 8)), -0.2, 0.2)), 0.0001296997, 0.12988281).astype(jnp.bfloat16)
    tile_mask = touch_ends((jax.random.randint(seeds[1], (NT, NT), 0, 2) < 1).astype(jnp.int32), jax.random.fold_in(seeds[1], 1), 0, 1)
    keep_mask = touch_ends((jax.random.randint(seeds[2], (NT, NT), 0, 4) < 3).astype(jnp.int32), jax.random.fold_in(seeds[2], 1), 0, 1)
    thr_index = touch_ends(jax.random.randint(seeds[3], (ORDER,), 0, 10), jax.random.fold_in(seeds[3], 1), 0, 9).astype(jnp.int32)
    return {"values": values, "tile_mask": tile_mask, "keep_mask": keep_mask, "thr_index": thr_index}


def reference(values, tile_mask, keep_mask, thr_index):
    matrix = (values.reshape(NT, TB, NT, TB) * tile_mask[:, None, :, None].astype(jnp.bfloat16)).reshape(ORDER, ORDER)
    product = jnp.dot(matrix, matrix, preferred_element_type=jnp.float32)
    col_means = jnp.sum(product, axis=0) / ORDER
    thresholds = 0.125 * thr_index.astype(jnp.float32)
    kept_cells = jnp.broadcast_to(keep_mask[:, None, :, None].astype(jnp.float32), (NT, TB, NT, TB)).reshape(ORDER, ORDER)
    pruned = jnp.maximum(product - thresholds * col_means, 0.0) * kept_cells
    col_totals = jnp.sum(pruned, axis=0) / ORDER
    return (pruned / jnp.maximum(col_totals, 0.1)).astype(jnp.bfloat16)
```

```python
import functools

import jax
import jax.numpy as jnp
from jax import lax
from jax.experimental import pallas as pl
from jax.experimental.pallas import tpu as pltpu
from jax.sharding import PartitionSpec as P

TB = 128
CORES = 2
CHUNKS = 4


def snake(index, width):
    line, spot = index // width, index % width
    return line * width + spot + (line % 2) * (width - 1 - 2 * spot)


def kernel(
    row_dev, col_dev, width, chunks, order,
    v_ref, tile_ref, keep_ref, thr_ref, acc, totals_ref,
    row_panel, col_panel, sums, stats,
    line_send, line_recv, pair_send, pair_recv, ring_send, ring_recv,
    sum_send, sum_recv, stat_send, stat_recv, loaded, load_sem, token,
):
    rows, cols = v_ref.shape
    step_rows = rows // chunks
    chips = col_dev // CORES
    half = row_dev // 2
    me_row, me_col = lax.axis_index("row"), lax.axis_index("col")
    z, core = me_col // CORES, me_col % CORES
    pos = snake(me_row, width)

    def ring_device(offset):
        return snake((pos + offset + row_dev) % row_dev, width)

    barrier = pltpu.get_barrier_semaphore()
    pl.semaphore_signal(barrier, inc=1, device_id={"col": z * CORES + 1 - core})
    peers = 1 + (z > 0).astype(jnp.int32) + (z < chips - 1).astype(jnp.int32)
    for offset in ((1, -1) if row_dev > 2 else (1,) * half):
        pl.semaphore_signal(barrier, inc=1, device_id={"row": ring_device(offset)})
        peers += 1

    @pl.when(z > 0)
    def _():
        pl.semaphore_signal(barrier, inc=1, device_id={"col": me_col - CORES})

    @pl.when(z < chips - 1)
    def _():
        pl.semaphore_signal(barrier, inc=1, device_id={"col": me_col + CORES})

    def load(q):
        spot = pl.ds(q * step_rows, step_rows)
        return pltpu.make_async_copy(v_ref.at[spot], loaded.at[spot], load_sem.at[q])

    for q in range(chunks):
        load(q).start()

    stored = tile_ref[...].astype(jnp.float32)
    kept = keep_ref[...].astype(jnp.float32)
    height = min(step_rows, TB)
    for lo in range(0, rows, height):
        if lo % step_rows == 0:
            load(lo // step_rows).wait()
        for b in range(cols // TB):
            r, c = slice(lo, lo + height), slice(b * TB, (b + 1) * TB)
            scale = jnp.broadcast_to(stored[b : b + 1, lo // TB : lo // TB + 1], (height, TB))
            tile = (loaded[r, c].astype(jnp.float32) * scale).astype(jnp.bfloat16)
            row_panel[me_col, r, c] = tile
            col_panel[pl.ds(pl.multiple_of(me_row * rows + lo, height), height), c] = tile

    pl.semaphore_wait(barrier, peers)

    def row_part(block, q):
        return row_panel.at[block, pl.ds(q * step_rows, step_rows)]

    def line_copy(zi, q, to_right):
        part = row_part(zi * CORES + core, q)
        return pltpu.make_async_remote_copy(
            src_ref=part, dst_ref=part,
            send_sem=line_send.at[to_right, zi, q], recv_sem=line_recv.at[zi, q],
            device_id={"col": me_col + (CORES if to_right else -CORES)},
        )

    def pair_copy(zi, q, lane):
        part = row_part(zi * CORES + lane, q)
        return pltpu.make_async_remote_copy(
            src_ref=part, dst_ref=part,
            send_sem=pair_send.at[zi, q], recv_sem=pair_recv.at[zi, q],
            device_id={"col": z * CORES + 1 - core},
        )

    def ring_copy(owner, q, to_right):
        start = pl.multiple_of(owner * rows + q * step_rows, step_rows)
        part = col_panel.at[pl.ds(start, step_rows)]
        return pltpu.make_async_remote_copy(
            src_ref=part, dst_ref=part,
            send_sem=ring_send.at[to_right, owner, q], recv_sem=ring_recv.at[owner, q],
            device_id={"row": ring_device(1 if to_right else -1)},
        )

    def on_ring(d, q, to_right):
        if d < half:
            return True
        return d == half and (q < chunks // 2) == bool(to_right)

    def relay(zi, q, to_right, wait):
        if wait:
            line_copy(zi, q, to_right).wait_recv()
        go = (z < chips - 1) if to_right else (z > 0)

        @pl.when(go)
        def _():
            line_copy(zi, q, to_right).start()

    for q in range(chunks):
        for to_right in (1, 0):
            relay(z, q, to_right, False)
            if on_ring(1, q, to_right):
                ring_copy(me_row, q, to_right).start()
        pair_copy(z, q, core).start()

    for to_right in (1, 0):
        first, end = (0, chips - 1) if to_right else (chips - 1, 0)

        @pl.when(z != first)
        def _():
            pl.semaphore_wait(token.at[to_right], 1)

        @pl.when(z != end)
        def _():
            pl.semaphore_signal(
                token.at[to_right], inc=1,
                device_id={"col": me_col + (CORES if to_right else -CORES)},
            )

    def line_step(t, q):
        for to_right in (1, 0):
            valid = (z >= t) if to_right else (z + t < chips)
            zi = z - t if to_right else z + t
            if t < chips:
                @pl.when(valid)
                def _():
                    relay(zi, q, to_right, True)
                    pair_copy(zi, q, core).start()

    def ring_step(t, q):
        for to_right in (1, 0):
            if on_ring(t, q, to_right):
                owner = ring_device(-t if to_right else t)
                ring_copy(owner, q, to_right).wait_recv()
                if on_ring(t + 1, q, to_right):
                    ring_copy(owner, q, to_right).start()

    def stat_copy(d):
        return pltpu.make_async_remote_copy(
            src_ref=stats.at[0], dst_ref=stats.at[d],
            send_sem=stat_send.at[d], recv_sem=stat_recv.at[d],
            device_id={"col": (me_col + d) % col_dev},
        )

    def send_stats():
        total = jnp.zeros((1, cols), jnp.float32)
        for i in range(row_dev):
            block = col_panel[i * rows : (i + 1) * rows].astype(jnp.float32)
            total += jnp.sum(block, axis=0, keepdims=True)
        stats[0] = total
        for d in range(1, col_dev):
            stat_copy(d).start()

    def product_sums():
        total = jnp.zeros((1, cols), jnp.float32)
        for d in range(col_dev):
            if d:
                stat_copy(d).wait()
            block = (me_col - d + col_dev) % col_dev
            inner = pl.ds(pl.multiple_of(block * cols, cols), cols)
            rest, terms = stats[d], []
            for _ in range(3):
                term = rest.astype(jnp.bfloat16).astype(jnp.float32)
                rest = rest - term
                terms.append(jnp.broadcast_to(term, (8, cols)))
            spread = jnp.dot(
                jnp.concatenate(terms, axis=0).astype(jnp.bfloat16), col_panel[inner],
                preferred_element_type=jnp.float32,
            )
            total += spread[16:17] + spread[8:9] + spread[0:1]
        return total

    def compute(zi, q, first=False):
        spot = pl.ds(pl.multiple_of(q * step_rows, step_rows), step_rows)
        total = None
        for lane in range(CORES):
            block = zi * CORES + lane
            inner = pl.ds(pl.multiple_of(block * cols, cols), cols)
            term = jnp.dot(
                row_panel[block, spot], col_panel[inner], preferred_element_type=jnp.float32
            )
            total = term if total is None else total + term
        if first:
            acc[spot] = total
        else:
            acc[spot] += total

    def take(zi, q, first=False):
        pair_copy(zi, q, 1 - core).wait_recv()
        compute(zi, q, first)

    def sides(t):
        return ((z >= t, z - t), (z + t < chips, z + t))

    def bulk(upto):
        @pl.loop(0, chunks)
        def _(q):
            take(z, q, True)
            for t in range(1, min(upto, chips - 1) + 1):
                for valid, zi in sides(t):
                    @pl.when(valid)
                    def _():
                        take(zi, q)

    def prune(q, cut):
        parts = []
        for b in range(cols // TB):
            c = slice(b * TB, (b + 1) * TB)
            part = jnp.zeros((1, TB), jnp.float32)
            for lo in range(q * step_rows, (q + 1) * step_rows, min(step_rows, TB)):
                r = slice(lo, lo + min(step_rows, TB))
                keep = jnp.broadcast_to(kept[b : b + 1, lo // TB : lo // TB + 1], (r.stop - lo, TB))
                pruned = jnp.maximum(acc[r, c] - cut[:, c], 0.0) * keep
                acc[r, c] = pruned
                part += jnp.sum(pruned, axis=0, keepdims=True)
            parts.append(part)
        return jnp.concatenate(parts, axis=1)

    def cuts():
        return 0.125 * thr_ref[...].astype(jnp.float32) * (product_sums() / order)

    part = jnp.zeros((1, cols), jnp.float32)
    last = max(chips - 1, half)
    if half == 0:
        send_stats()
        bulk(0)
    for t in range(1, last + 1):
        if t == half:
            for q in range(chunks):
                ring_step(t, q)
            send_stats()
            for q in range(chunks):
                line_step(t, q)
            bulk(t)
        else:
            if t == last and t > half:
                cut = cuts()
            for q in range(chunks):
                line_step(t, q)
                if t < half:
                    ring_step(t, q)
                else:
                    for valid, zi in sides(t):
                        @pl.when(valid)
                        def _():
                            take(zi, q)
                    if t == last:
                        part += prune(q, cut)
    if last <= half:
        cut = cuts()
        for q in range(chunks):
            part += prune(q, cut)

    sums[0] = part

    def sum_copy(d):
        return pltpu.make_async_remote_copy(
            src_ref=sums.at[0], dst_ref=sums.at[d],
            send_sem=sum_send.at[d], recv_sem=sum_recv.at[d],
            device_id={"row": (me_row + d) % row_dev},
        )

    for d in range(1, row_dev):
        sum_copy(d).start()
    for d in range(1, row_dev):
        sum_copy(d).wait()
        part += sums[d]
    totals_ref[...] = 1.0 / jnp.maximum(part / order, 0.1)

    for q in range(chunks):
        for zi in range(chips):
            pair_copy(zi, q, core).wait_send()

            @pl.when((z < chips - 1) & (z >= zi))
            def _():
                line_copy(zi, q, 1).wait_send()

            @pl.when((z > 0) & (z <= zi))
            def _():
                line_copy(zi, q, 0).wait_send()
        for d in range(0, half):
            for to_right in (1, 0):
                if on_ring(d + 1, q, to_right):
                    owner = ring_device(-d if to_right else d)
                    ring_copy(owner, q, to_right).wait_send()


def cut_rows(lo, hi):
    while lo < hi:
        stop = min(hi, (lo // TB + 1) * TB)
        yield lo, stop
        lo = stop


def near_kernel(
    width, bounds, order,
    v_ref, tile_ref, keep_ref, thr_ref, acc, scale_ref,
    row_panel, col_panel, far, done, done_in, ahead,
    row_sums, stats, sums, far_sums, ahead_sums, notes, loaded,
    line_send, line_recv, pair_send, pair_recv, ring_send, ring_recv,
    far_send, far_recv, far_line_send, far_line_recv,
    row_send, row_recv, stat_send, stat_recv, sum_send, sum_recv,
    far_sum_send, far_sum_recv, ahead_send, ahead_recv,
    note_send, note_recv, done_send, done_recv, load_sem,
):
    rows, cols = v_ref.shape
    row_dev, col_dev, chips = row_sums.shape[0], stats.shape[0], stats.shape[0] // CORES
    chunks = len(bounds) - 1
    me_row, me_col = lax.axis_index("row"), lax.axis_index("col")
    z, core = me_col // CORES, me_col % CORES
    pos = snake(me_row, width)
    on_right = z >= chips // 2
    end = jnp.where(on_right, chips - 1, 0)
    out = jnp.where(on_right, 1, -1)
    near, over, other = end - out, end - 2 * out, end - 3 * out
    is_end = z == end
    is_near = z == near

    def ring_device(offset):
        return snake((pos + offset + row_dev) % row_dev, width)

    opposite = ring_device(2)

    barrier = pltpu.get_barrier_semaphore()
    for d in range(1, row_dev):
        pl.semaphore_signal(barrier, inc=1, device_id={"row": (me_row + d) % row_dev})
    for d in range(1, col_dev):
        pl.semaphore_signal(barrier, inc=1, device_id={"col": (me_col + d) % col_dev})

    def span(q):
        return pl.ds(bounds[q], bounds[q + 1] - bounds[q])

    def block_rows(owner, q):
        return pl.ds(pl.multiple_of(owner * rows + bounds[q], 16), bounds[q + 1] - bounds[q])

    def load(q):
        return pltpu.make_async_copy(v_ref.at[span(q)], loaded.at[span(q)], load_sem.at[q])

    for q in range(chunks):
        load(q).start()

    stored = tile_ref[...].astype(jnp.float32)
    kept = keep_ref[...].astype(jnp.float32)
    tile_sums = [jnp.zeros((1, TB), jnp.float32) for _ in range(cols // TB)]
    for q in range(chunks):
        load(q).wait()
        for lo, hi in cut_rows(bounds[q], bounds[q + 1]):
            for b in range(cols // TB):
                r, c = slice(lo, hi), slice(b * TB, (b + 1) * TB)
                scale = jnp.broadcast_to(stored[b : b + 1, lo // TB : lo // TB + 1], (hi - lo, TB))
                tile = loaded[r, c].astype(jnp.float32) * scale
                tile_sums[b] += jnp.sum(tile, axis=0, keepdims=True)
                tile = tile.astype(jnp.bfloat16)
                row_panel[me_col, r, c] = tile
                col_panel[pl.ds(pl.multiple_of(me_row * rows + lo, 16), hi - lo), c] = tile
    row_sums[0] = jnp.concatenate(tile_sums, axis=1)

    pl.semaphore_wait(barrier, row_dev + col_dev - 2)

    def line(zi, q, outward):
        part = row_panel.at[zi * CORES + core, span(q)]
        return pltpu.make_async_remote_copy(
            src_ref=part, dst_ref=part,
            send_sem=line_send.at[outward, zi, q], recv_sem=line_recv.at[zi, q],
            device_id={"col": me_col + (CORES if outward else -CORES) * out},
        )

    def pair(zi, q, lane):
        part = row_panel.at[zi * CORES + lane, span(q)]
        return pltpu.make_async_remote_copy(
            src_ref=part, dst_ref=part,
            send_sem=pair_send.at[zi, q], recv_sem=pair_recv.at[zi, q],
            device_id={"col": z * CORES + 1 - core},
        )

    def ring(owner, q, to_right):
        part = col_panel.at[block_rows(owner, q)]
        return pltpu.make_async_remote_copy(
            src_ref=part, dst_ref=part,
            send_sem=ring_send.at[to_right, owner, q], recv_sem=ring_recv.at[owner, q],
            device_id={"row": ring_device(1 if to_right else -1)},
        )

    def far_ring(q, to_right):
        return pltpu.make_async_remote_copy(
            src_ref=row_panel.at[end * CORES + core, span(q)],
            dst_ref=far.at[block_rows(me_row, q)],
            send_sem=far_send.at[to_right, q], recv_sem=far_recv.at[to_right, q],
            device_id={"row": ring_device(1 if to_right else -1)},
        )

    def far_line(q):
        part = block_rows(opposite, q)
        return pltpu.make_async_remote_copy(
            src_ref=col_panel.at[part], dst_ref=far.at[part],
            send_sem=far_line_send.at[q], recv_sem=far_line_recv.at[q],
            device_id={"col": me_col - CORES * out},
        )

    def row_sum_copy(d):
        return pltpu.make_async_remote_copy(
            src_ref=row_sums.at[0], dst_ref=row_sums.at[d],
            send_sem=row_send.at[d], recv_sem=row_recv.at[d],
            device_id={"row": (me_row + d) % row_dev},
        )

    def stat_copy(d):
        return pltpu.make_async_remote_copy(
            src_ref=stats.at[0], dst_ref=stats.at[d],
            send_sem=stat_send.at[d], recv_sem=stat_recv.at[d],
            device_id={"col": (me_col + d) % col_dev},
        )

    def sum_copy(d):
        return pltpu.make_async_remote_copy(
            src_ref=sums.at[0], dst_ref=sums.at[d],
            send_sem=sum_send.at[d], recv_sem=sum_recv.at[d],
            device_id={"row": (me_row + d) % row_dev},
        )

    def far_sum_copy(d):
        return pltpu.make_async_remote_copy(
            src_ref=sums.at[0], dst_ref=far_sums.at[d],
            send_sem=far_sum_send.at[d], recv_sem=far_sum_recv.at[d],
            device_id={"row": (me_row + d) % row_dev, "col": me_col - CORES * out},
        )

    def ahead_copy():
        return pltpu.make_async_remote_copy(
            src_ref=ahead_sums.at[0], dst_ref=ahead_sums.at[1],
            send_sem=ahead_send.at[0], recv_sem=ahead_recv.at[0],
            device_id={"col": me_col + CORES * out},
        )

    def note_copy():
        return pltpu.make_async_remote_copy(
            src_ref=notes.at[0], dst_ref=notes.at[1],
            send_sem=note_send.at[0], recv_sem=note_recv.at[0],
            device_id={"col": me_col - CORES * out},
        )

    halves = (0, done.shape[0] // 32 * 16, done.shape[0])

    def done_copy(h):
        part = pl.ds(halves[h], halves[h + 1] - halves[h])
        return pltpu.make_async_remote_copy(
            src_ref=done.at[part], dst_ref=done_in.at[part],
            send_sem=done_send.at[h], recv_sem=done_recv.at[h],
            device_id={"col": me_col + CORES * out},
        )

    def relays(q, to_right):
        return (q % 2 == 0) == bool(to_right)

    def own_ring(q):
        for to_right in (1, 0):
            ring(me_row, q, to_right).start()

    def ring_wait(q):
        for to_right in (1, 0):
            ring(ring_device(-1 if to_right else 1), q, to_right).wait_recv()

    def ring_relay(q):
        for to_right in (1, 0):
            if relays(q, to_right):
                ring(ring_device(-1 if to_right else 1), q, to_right).start()

    def ring_last(q):
        ring(opposite, q, 1 if relays(q, 1) else 0).wait_recv()

    ahead_of = chunks - 1
    base = bounds[ahead_of]
    raw = range(ahead_of)

    for d in range(1, row_dev):
        row_sum_copy(d).start()

    @pl.when(is_end)
    def _():
        for q in range(chunks):
            line(end, q, 0).start()
            if q < 2:
                own_ring(q)
            if q in raw:
                pair(end, q, core).start()

    @pl.when(is_near)
    def _():
        for q in range(chunks):
            if q < 2:
                line(near, q, 0).start()
                own_ring(q)
            if q in raw:
                line(near, q, 1).start()
            pair(near, q, core).start()

    def send_stats():
        for d in range(1, row_dev):
            row_sum_copy(d).wait()
        total = row_sums[0]
        for d in range(1, row_dev):
            total += row_sums[d]
        stats[0] = total
        for d in range(1, col_dev):
            stat_copy(d).start()

    def wait_stats():
        for d in range(1, col_dev):
            stat_copy(d).wait()

    def inner(owner, lane):
        return pl.ds(pl.multiple_of((owner * CORES + lane) * cols, cols), cols)

    def product_sums(owners, lanes=range(CORES)):
        total = jnp.zeros((1, cols), jnp.float32)
        for owner in owners:
            for lane in lanes:
                rest = stats[(me_col - owner * CORES - lane + col_dev) % col_dev]
                terms = []
                for _ in range(3):
                    term = rest.astype(jnp.bfloat16).astype(jnp.float32)
                    rest = rest - term
                    terms.append(jnp.broadcast_to(term, (8, cols)))
                spread = jnp.dot(
                    jnp.concatenate(terms, axis=0).astype(jnp.bfloat16),
                    col_panel[inner(owner, lane)], preferred_element_type=jnp.float32,
                )
                total += spread[16:17] + spread[8:9] + spread[0:1]
        return total

    def cuts(total):
        return 0.125 * thr_ref[...].astype(jnp.float32) * (total / order)

    def product(zis, q, lanes=range(CORES)):
        total = None
        for zi in zis:
            for lane in lanes:
                term = jnp.dot(
                    row_panel[zi * CORES + lane, span(q)], col_panel[inner(zi, lane)],
                    preferred_element_type=jnp.float32,
                )
                total = term if total is None else total + term
        return total

    def prune(q, cut):
        parts = []
        for b in range(cols // TB):
            c = slice(b * TB, (b + 1) * TB)
            part = jnp.zeros((1, TB), jnp.float32)
            for lo, hi in cut_rows(bounds[q], bounds[q + 1]):
                keep = jnp.broadcast_to(kept[b : b + 1, lo // TB : lo // TB + 1], (hi - lo, TB))
                pruned = jnp.maximum(acc[lo:hi, c] - cut[:, c], 0.0) * keep
                acc[lo:hi, c] = pruned
                part += jnp.sum(pruned, axis=0, keepdims=True)
            parts.append(part)
        return jnp.concatenate(parts, axis=1)

    def normal(total):
        return 1.0 / jnp.maximum(total / order, 0.1)

    def arrive(zi, q, relay):
        line(zi, q, 1).wait_recv()
        if relay is not None:
            line(zi, q, relay).start()
        pair(zi, q, core).start()

    def met(zi, q):
        pair(zi, q, 1 - core).wait_recv()

    @pl.when(is_end)
    def _():
        ring_wait(0)
        ring_relay(0)
        own_ring(2)
        send_stats()
        ring_wait(1)
        ring_relay(1)
        own_ring(3)
        arrive(near, 0, None)
        arrive(near, 1, None)
        ring_last(0)
        far_line(0).start()
        ring_wait(2)
        ring_relay(2)
        arrive(near, 2, None)
        ring_last(1)
        far_line(1).start()
        ring_wait(3)
        ring_relay(3)
        arrive(over, 0, None)
        arrive(over, 1, None)
        ring_last(2)
        far_line(2).start()
        ring_last(3)
        far_line(3).start()
        arrive(other, 0, None)
        wait_stats()
        cut = cuts(product_sums(range(chips)))
        note = [cut]
        for t in range(base // TB, base // TB + 7):
            t = min(t, rows // TB - 1)
            line_of = [
                jnp.broadcast_to(kept[b : b + 1, t : t + 1], (1, TB)) for b in range(cols // TB)
            ]
            note.append(jnp.concatenate(line_of, axis=1))
        notes[0] = jnp.concatenate(note, axis=0)
        for q in raw:
            met(end, q)
            met(near, q)
        acc[span(2)] = product((end, near), 2)
        note_copy().start()
        met(over, 0)
        met(over, 1)
        acc[span(1)] = product((end, near, over), 1)
        met(other, 0)
        acc[span(0)] = product((end, near, over, other), 0)
        part = prune(0, cut)
        arrive(over, 2, None)
        arrive(other, 1, None)
        met(over, 2)
        acc[span(2)] += product((over,), 2)
        met(other, 1)
        acc[span(1)] += product((other,), 1)
        part += prune(1, cut)
        arrive(other, 2, None)
        met(other, 2)
        acc[span(2)] += product((other,), 2)
        part += prune(2, cut)
        ahead_copy().wait_recv()
        sums[0] = part + ahead_sums[1]
        for d in range(row_dev):
            far_sum_copy(d).start()
            if d:
                sum_copy(d).start()
        part = sums[0]
        for d in range(1, row_dev):
            sum_copy(d).wait()
            part += sums[d]
        scale_ref[0:1] = jnp.ones((1, cols), jnp.float32)
        scale_ref[1:2] = normal(part)
        for h in range(2):
            done_copy(h).wait_recv()
            part = slice(halves[h], halves[h + 1])
            acc[base + halves[h] : base + halves[h + 1]] = done_in[part].astype(jnp.float32)
        note_copy().wait_send()
        for d in range(row_dev):
            far_sum_copy(d).wait_send()
        for q in range(chunks):
            line(end, q, 0).wait_send()
            far_line(q).wait_send()
            if q in raw:
                for zi in range(chips):
                    pair(zi, q, core).wait_send()

    @pl.when(is_near)
    def _():
        def from_end(q):
            arrive(end, q, 0)
            if q % 2 == 0:
                line(near, 2 + q // 2, 0).start()
            for to_right in (1, 0):
                far_ring(q, to_right).start()
            if q < 2:
                own_ring(q + 2)

        def from_over(zi, q):
            arrive(zi, q, 1 if q in raw else None)

        beside = (me_row, ring_device(1), ring_device(-1))
        from_end(0)
        send_stats()
        from_over(over, 0)
        from_end(1)
        from_over(over, 1)
        from_end(2)
        from_over(other, 0)
        from_end(3)
        ring_wait(0)
        ring_relay(0)
        ring_wait(1)
        ring_relay(1)
        from_over(over, 2)
        ring_wait(2)
        ring_relay(2)
        from_over(other, 1)
        ring_wait(3)
        ring_relay(3)
        from_over(other, 2)
        for q in raw:
            for zi in beside:
                met(zi, q)
            acc[span(q)] = product(beside, q)
        from_over(over, 3)
        from_over(other, 3)
        for zi in (*beside, opposite):
            met(zi, ahead_of)
        for q in range(chunks):
            for to_right in (1, 0):
                far_ring(q, to_right).wait_recv()
        total = None
        for lane in range(CORES):
            for owner in beside:
                source = (
                    row_panel[end * CORES + core, lane * cols : (lane + 1) * cols]
                    if owner is me_row else far[inner(owner, lane)]
                )
                term = jnp.dot(
                    row_panel[owner * CORES + lane, span(ahead_of)], source,
                    preferred_element_type=jnp.float32,
                )
                total = term if total is None else total + term
        ahead[...] = total
        for q in range(chunks):
            far_line(q).wait_recv()
        total = ahead[...]
        for lane in range(CORES):
            total += jnp.dot(
                row_panel[opposite * CORES + lane, span(ahead_of)], far[inner(opposite, lane)],
                preferred_element_type=jnp.float32,
            )
        ahead[...] = total
        note_copy().wait_recv()
        parts = jnp.zeros((1, cols), jnp.float32)
        for lo, hi in cut_rows(base, rows):
            tile = lo // TB - base // TB + 1
            pruned = jnp.maximum(ahead[lo - base : hi - base] - notes[1, 0:1], 0.0)
            pruned *= notes[1, tile : tile + 1]
            ahead[lo - base : hi - base] = pruned
            parts += jnp.sum(pruned, axis=0, keepdims=True)
        ahead_sums[0] = parts
        ahead_copy().start()
        acc[span(ahead_of)] = product(beside, ahead_of)
        wait_stats()
        head = product_sums(beside)
        part = jnp.zeros((1, cols), jnp.float32)
        for d in range(row_dev):
            far_sum_copy(d).wait_recv()
            part += far_sums[d]
        scale = normal(part)
        for h in range(2):
            done[halves[h] : halves[h + 1]] = (
                ahead[halves[h] : halves[h + 1]] * scale
            ).astype(jnp.bfloat16)
        for h in range(2):
            done_copy(h).start()
        for q in raw:
            met(opposite, q)
        ring_last(0)
        ring_last(1)
        for q in range(chunks):
            acc[span(q)] += product((opposite,), q, (0,))
        head += product_sums((opposite,), (0,))
        ring_last(2)
        ring_last(3)
        cut = cuts(head + product_sums((opposite,), (1,)))
        part = jnp.zeros((1, cols), jnp.float32)
        for q in range(chunks):
            acc[span(q)] += product((opposite,), q, (1,))
            part += prune(q, cut)
        sums[0] = part
        for d in range(1, row_dev):
            sum_copy(d).start()
        for d in range(1, row_dev):
            sum_copy(d).wait()
            part += sums[d]
        scale_ref[...] = jnp.broadcast_to(normal(part), scale_ref.shape)
        ahead_copy().wait_send()
        for h in range(2):
            done_copy(h).wait_send()
        for q in range(chunks):
            line(near, q, 0).wait_send()
            line(end, q, 0).wait_send()
            if q in raw:
                for zi in (near, over, other):
                    line(zi, q, 1).wait_send()
            for zi in range(chips):
                pair(zi, q, core).wait_send()
            for to_right in (1, 0):
                far_ring(q, to_right).wait_send()

    for q in range(chunks):
        for to_right in (1, 0):
            ring(me_row, q, to_right).wait_send()
            if relays(q, to_right):
                ring(ring_device(-1 if to_right else 1), q, to_right).wait_send()


def near_call(values, tile_mask, keep_mask, thr_index, *, row_dev, col_dev, width):
    rows, cols = values.shape
    chips = col_dev // CORES
    base = rows * 11 // 16 // 16 * 16
    bounds = (0, cols // 32 * 16, cols, base, rows)
    ahead = rows - base
    chunks = len(bounds) - 1
    dma = pltpu.SemaphoreType.DMA
    vmem = pl.BlockSpec(memory_space=pltpu.VMEM)
    pruned, scale = pl.pallas_call(
        functools.partial(near_kernel, width, bounds, rows * row_dev),
        out_shape=(
            pltpu.VMEM((rows, cols), jnp.float32),
            pltpu.VMEM((2, cols), jnp.float32),
        ),
        in_specs=[pl.BlockSpec(memory_space=pl.ANY)] + [vmem] * 3,
        out_specs=(vmem, vmem),
        scratch_shapes=[
            pltpu.VMEM((col_dev, rows, cols), jnp.bfloat16),
            pltpu.VMEM((row_dev * rows, cols), jnp.bfloat16),
            pltpu.VMEM((row_dev * rows, cols), jnp.bfloat16),
            pltpu.VMEM((ahead, cols), jnp.bfloat16),
            pltpu.VMEM((ahead, cols), jnp.bfloat16),
            pltpu.VMEM((ahead, cols), jnp.float32),
            pltpu.VMEM((row_dev, 1, cols), jnp.float32),
            pltpu.VMEM((col_dev, 1, cols), jnp.float32),
            pltpu.VMEM((row_dev, 1, cols), jnp.float32),
            pltpu.VMEM((row_dev, 1, cols), jnp.float32),
            pltpu.VMEM((2, 1, cols), jnp.float32),
            pltpu.VMEM((2, 8, cols), jnp.float32),
            pltpu.VMEM((rows, cols), jnp.bfloat16),
            dma((2, chips, chunks)), dma((chips, chunks)),
            dma((chips, chunks)), dma((chips, chunks)),
            dma((2, row_dev, chunks)), dma((row_dev, chunks)),
            dma((2, chunks)), dma((2, chunks)),
            dma((chunks,)), dma((chunks,)),
            dma((row_dev,)), dma((row_dev,)),
            dma((col_dev,)), dma((col_dev,)),
            dma((row_dev,)), dma((row_dev,)),
            dma((row_dev,)), dma((row_dev,)),
            dma((1,)), dma((1,)),
            dma((1,)), dma((1,)),
            dma((2,)), dma((2,)),
            dma((chunks,)),
        ],
        compiler_params=pltpu.CompilerParams(
            collective_id=0, has_side_effects=True,
            vmem_limit_bytes=63 * 2**20 - 4 * rows * cols + 2**19,
        ),
    )(values, tile_mask.T, keep_mask.T, thr_index.reshape(1, cols))
    early = lax.broadcasted_iota(jnp.int32, (rows, 1), 0) >= base
    return (pruned * jnp.where(early, scale[0:1], scale[1:2])).astype(jnp.bfloat16)


def on_device(values, tile_mask, keep_mask, thr_index, *, row_dev, col_dev):
    rows, cols = values.shape
    width = max(w for w in range(1, row_dev + 1) if row_dev % w == 0 and w * w <= row_dev)
    chips = col_dev // CORES
    if chips == 4 and row_dev == 4 and rows == CORES * cols:
        return near_call(
            values, tile_mask, keep_mask, thr_index, row_dev=row_dev, col_dev=col_dev, width=width
        )
    dma = pltpu.SemaphoreType.DMA
    vmem = pl.BlockSpec(memory_space=pltpu.VMEM)
    pruned, scale = pl.pallas_call(
        functools.partial(kernel, row_dev, col_dev, width, CHUNKS, rows * row_dev),
        out_shape=(
            pltpu.VMEM((rows, cols), jnp.float32),
            jax.ShapeDtypeStruct((1, cols), jnp.float32),
        ),
        in_specs=[pl.BlockSpec(memory_space=pl.ANY)] + [vmem] * 3,
        out_specs=(vmem, vmem),
        scratch_shapes=[
            pltpu.VMEM((col_dev, rows, cols), jnp.bfloat16),
            pltpu.VMEM((row_dev * rows, cols), jnp.bfloat16),
            pltpu.VMEM((row_dev, 1, cols), jnp.float32),
            pltpu.VMEM((col_dev, 1, cols), jnp.float32),
            dma((2, chips, CHUNKS)),
            dma((chips, CHUNKS)),
            dma((chips, CHUNKS)),
            dma((chips, CHUNKS)),
            dma((2, row_dev, CHUNKS)),
            dma((row_dev, CHUNKS)),
            dma((row_dev,)),
            dma((row_dev,)),
            dma((col_dev,)),
            dma((col_dev,)),
            pltpu.VMEM((rows, cols), jnp.bfloat16),
            dma((CHUNKS,)),
            pltpu.SemaphoreType.REGULAR((2,)),
        ],
        compiler_params=pltpu.CompilerParams(
            collective_id=0, has_side_effects=True,
            vmem_limit_bytes=63 * 2**20 - 4 * rows * cols + 2**19,
        ),
    )(values, tile_mask.T, keep_mask.T, thr_index.reshape(1, cols))
    return (pruned * scale).astype(jnp.bfloat16)


def solution(mesh):
    return jax.shard_map(
        functools.partial(on_device, row_dev=mesh.shape["row"], col_dev=mesh.shape["col"]),
        mesh=mesh,
        in_specs=(P("row", "col"), P("row", "col"), P("row", "col"), P("col")),
        out_specs=P("row", "col"),
        check_vma=False,
    )
```

```python
import functools

import jax
import jax.numpy as jnp
from jax import lax
from jax.experimental import pallas as pl
from jax.experimental.pallas import tpu as pltpu
from jax.sharding import PartitionSpec as P

TB = 128
CORES = 2
CHUNKS = 4


def snake(index, width):
    line, spot = index // width, index % width
    return line * width + spot + (line % 2) * (width - 1 - 2 * spot)


def kernel(
    row_dev, col_dev, width, chunks, order,
    v_ref, tile_ref, keep_ref, thr_ref, acc, totals_ref,
    row_panel, col_panel, sums, stats,
    line_send, line_recv, pair_send, pair_recv, ring_send, ring_recv,
    sum_send, sum_recv, stat_send, stat_recv, loaded, load_sem, token,
):
    rows, cols = v_ref.shape
    step_rows = rows // chunks
    chips = col_dev // CORES
    half = row_dev // 2
    me_row, me_col = lax.axis_index("row"), lax.axis_index("col")
    z, core = me_col // CORES, me_col % CORES
    pos = snake(me_row, width)

    def ring_device(offset):
        return snake((pos + offset + row_dev) % row_dev, width)

    barrier = pltpu.get_barrier_semaphore()
    pl.semaphore_signal(barrier, inc=1, device_id={"col": z * CORES + 1 - core})
    peers = 1 + (z > 0).astype(jnp.int32) + (z < chips - 1).astype(jnp.int32)
    for offset in ((1, -1) if row_dev > 2 else (1,) * half):
        pl.semaphore_signal(barrier, inc=1, device_id={"row": ring_device(offset)})
        peers += 1

    @pl.when(z > 0)
    def _():
        pl.semaphore_signal(barrier, inc=1, device_id={"col": me_col - CORES})

    @pl.when(z < chips - 1)
    def _():
        pl.semaphore_signal(barrier, inc=1, device_id={"col": me_col + CORES})

    def load(q):
        spot = pl.ds(q * step_rows, step_rows)
        return pltpu.make_async_copy(v_ref.at[spot], loaded.at[spot], load_sem.at[q])

    for q in range(chunks):
        load(q).start()

    stored = tile_ref[...].astype(jnp.float32)
    kept = keep_ref[...].astype(jnp.float32)
    height = min(step_rows, TB)
    for lo in range(0, rows, height):
        if lo % step_rows == 0:
            load(lo // step_rows).wait()
        for b in range(cols // TB):
            r, c = slice(lo, lo + height), slice(b * TB, (b + 1) * TB)
            scale = jnp.broadcast_to(stored[b : b + 1, lo // TB : lo // TB + 1], (height, TB))
            tile = (loaded[r, c].astype(jnp.float32) * scale).astype(jnp.bfloat16)
            row_panel[me_col, r, c] = tile
            col_panel[pl.ds(pl.multiple_of(me_row * rows + lo, height), height), c] = tile

    pl.semaphore_wait(barrier, peers)

    def row_part(block, q):
        return row_panel.at[block, pl.ds(q * step_rows, step_rows)]

    def line_copy(zi, q, to_right):
        part = row_part(zi * CORES + core, q)
        return pltpu.make_async_remote_copy(
            src_ref=part, dst_ref=part,
            send_sem=line_send.at[to_right, zi, q], recv_sem=line_recv.at[zi, q],
            device_id={"col": me_col + (CORES if to_right else -CORES)},
        )

    def pair_copy(zi, q, lane):
        part = row_part(zi * CORES + lane, q)
        return pltpu.make_async_remote_copy(
            src_ref=part, dst_ref=part,
            send_sem=pair_send.at[zi, q], recv_sem=pair_recv.at[zi, q],
            device_id={"col": z * CORES + 1 - core},
        )

    def ring_copy(owner, q, to_right):
        start = pl.multiple_of(owner * rows + q * step_rows, step_rows)
        part = col_panel.at[pl.ds(start, step_rows)]
        return pltpu.make_async_remote_copy(
            src_ref=part, dst_ref=part,
            send_sem=ring_send.at[to_right, owner, q], recv_sem=ring_recv.at[owner, q],
            device_id={"row": ring_device(1 if to_right else -1)},
        )

    def on_ring(d, q, to_right):
        if d < half:
            return True
        return d == half and (q < chunks // 2) == bool(to_right)

    def relay(zi, q, to_right, wait):
        if wait:
            line_copy(zi, q, to_right).wait_recv()
        go = (z < chips - 1) if to_right else (z > 0)

        @pl.when(go)
        def _():
            line_copy(zi, q, to_right).start()

    for q in range(chunks):
        for to_right in (1, 0):
            relay(z, q, to_right, False)
            if on_ring(1, q, to_right):
                ring_copy(me_row, q, to_right).start()
        pair_copy(z, q, core).start()

    for to_right in (1, 0):
        first, end = (0, chips - 1) if to_right else (chips - 1, 0)

        @pl.when(z != first)
        def _():
            pl.semaphore_wait(token.at[to_right], 1)

        @pl.when(z != end)
        def _():
            pl.semaphore_signal(
                token.at[to_right], inc=1,
                device_id={"col": me_col + (CORES if to_right else -CORES)},
            )

    def line_step(t, q):
        for to_right in (1, 0):
            valid = (z >= t) if to_right else (z + t < chips)
            zi = z - t if to_right else z + t
            if t < chips:
                @pl.when(valid)
                def _():
                    relay(zi, q, to_right, True)
                    pair_copy(zi, q, core).start()

    def ring_step(t, q):
        for to_right in (1, 0):
            if on_ring(t, q, to_right):
                owner = ring_device(-t if to_right else t)
                ring_copy(owner, q, to_right).wait_recv()
                if on_ring(t + 1, q, to_right):
                    ring_copy(owner, q, to_right).start()

    def stat_copy(d):
        return pltpu.make_async_remote_copy(
            src_ref=stats.at[0], dst_ref=stats.at[d],
            send_sem=stat_send.at[d], recv_sem=stat_recv.at[d],
            device_id={"col": (me_col + d) % col_dev},
        )

    def send_stats():
        total = jnp.zeros((1, cols), jnp.float32)
        for i in range(row_dev):
            block = col_panel[i * rows : (i + 1) * rows].astype(jnp.float32)
            total += jnp.sum(block, axis=0, keepdims=True)
        stats[0] = total
        for d in range(1, col_dev):
            stat_copy(d).start()

    def product_sums():
        total = jnp.zeros((1, cols), jnp.float32)
        for d in range(col_dev):
            if d:
                stat_copy(d).wait()
            block = (me_col - d + col_dev) % col_dev
            inner = pl.ds(pl.multiple_of(block * cols, cols), cols)
            rest, terms = stats[d], []
            for _ in range(3):
                term = rest.astype(jnp.bfloat16).astype(jnp.float32)
                rest = rest - term
                terms.append(jnp.broadcast_to(term, (8, cols)))
            spread = jnp.dot(
                jnp.concatenate(terms, axis=0).astype(jnp.bfloat16), col_panel[inner],
                preferred_element_type=jnp.float32,
            )
            total += spread[16:17] + spread[8:9] + spread[0:1]
        return total

    def compute(zi, q, first=False):
        spot = pl.ds(pl.multiple_of(q * step_rows, step_rows), step_rows)
        total = None
        for lane in range(CORES):
            block = zi * CORES + lane
            inner = pl.ds(pl.multiple_of(block * cols, cols), cols)
            term = jnp.dot(
                row_panel[block, spot], col_panel[inner], preferred_element_type=jnp.float32
            )
            total = term if total is None else total + term
        if first:
            acc[spot] = total
        else:
            acc[spot] += total

    def take(zi, q, first=False):
        pair_copy(zi, q, 1 - core).wait_recv()
        compute(zi, q, first)

    def sides(t):
        return ((z >= t, z - t), (z + t < chips, z + t))

    def bulk(upto):
        @pl.loop(0, chunks)
        def _(q):
            take(z, q, True)
            for t in range(1, min(upto, chips - 1) + 1):
                for valid, zi in sides(t):
                    @pl.when(valid)
                    def _():
                        take(zi, q)

    def prune(q, cut):
        parts = []
        for b in range(cols // TB):
            c = slice(b * TB, (b + 1) * TB)
            part = jnp.zeros((1, TB), jnp.float32)
            for lo in range(q * step_rows, (q + 1) * step_rows, min(step_rows, TB)):
                r = slice(lo, lo + min(step_rows, TB))
                keep = jnp.broadcast_to(kept[b : b + 1, lo // TB : lo // TB + 1], (r.stop - lo, TB))
                pruned = jnp.maximum(acc[r, c] - cut[:, c], 0.0) * keep
                acc[r, c] = pruned
                part += jnp.sum(pruned, axis=0, keepdims=True)
            parts.append(part)
        return jnp.concatenate(parts, axis=1)

    def cuts():
        return 0.125 * thr_ref[...].astype(jnp.float32) * (product_sums() / order)

    part = jnp.zeros((1, cols), jnp.float32)
    last = max(chips - 1, half)
    if half == 0:
        send_stats()
        bulk(0)
    for t in range(1, last + 1):
        if t == half:
            for q in range(chunks):
                ring_step(t, q)
            send_stats()
            for q in range(chunks):
                line_step(t, q)
            bulk(t)
        else:
            if t == last and t > half:
                cut = cuts()
            for q in range(chunks):
                line_step(t, q)
                if t < half:
                    ring_step(t, q)
                else:
                    for valid, zi in sides(t):
                        @pl.when(valid)
                        def _():
                            take(zi, q)
                    if t == last:
                        part += prune(q, cut)
    if last <= half:
        cut = cuts()
        for q in range(chunks):
            part += prune(q, cut)

    sums[0] = part

    def sum_copy(d):
        return pltpu.make_async_remote_copy(
            src_ref=sums.at[0], dst_ref=sums.at[d],
            send_sem=sum_send.at[d], recv_sem=sum_recv.at[d],
            device_id={"row": (me_row + d) % row_dev},
        )

    for d in range(1, row_dev):
        sum_copy(d).start()
    for d in range(1, row_dev):
        sum_copy(d).wait()
        part += sums[d]
    totals_ref[...] = 1.0 / jnp.maximum(part / order, 0.1)

    for q in range(chunks):
        for zi in range(chips):
            pair_copy(zi, q, core).wait_send()

            @pl.when((z < chips - 1) & (z >= zi))
            def _():
                line_copy(zi, q, 1).wait_send()

            @pl.when((z > 0) & (z <= zi))
            def _():
                line_copy(zi, q, 0).wait_send()
        for d in range(0, half):
            for to_right in (1, 0):
                if on_ring(d + 1, q, to_right):
                    owner = ring_device(-d if to_right else d)
                    ring_copy(owner, q, to_right).wait_send()


def cut_rows(lo, hi):
    while lo < hi:
        stop = min(hi, (lo // TB + 1) * TB)
        yield lo, stop
        lo = stop


def near_kernel(
    width, bounds, split, order,
    v_ref, tile_ref, keep_ref, thr_ref, out_ref, acc,
    row_panel, col_panel, far, done, ahead,
    row_sums, stats, sums, ahead_sums, total_sums, notes, loaded,
    sent, small, line_recv, pair_recv, ring_recv, far_recv, load_sem,
):
    rows, cols = v_ref.shape
    row_dev, col_dev, chips = row_sums.shape[0], stats.shape[0], stats.shape[0] // CORES
    chunks = len(bounds) - 1
    ahead_of = chunks - 1
    base = bounds[ahead_of]
    raw = range(ahead_of)
    me_row, me_col = lax.axis_index("row"), lax.axis_index("col")
    z, core = me_col // CORES, me_col % CORES
    pos = snake(me_row, width)
    on_right = z >= chips // 2
    end = jnp.where(on_right, chips - 1, 0)
    out = jnp.where(on_right, 1, -1)
    near, over, other = end - out, end - 2 * out, end - 3 * out
    is_end = z == end
    is_near = z == near
    inward, outward = me_col - CORES * out, me_col + CORES * out

    def ring_device(offset):
        return snake((pos + offset + row_dev) % row_dev, width)

    opposite = ring_device(2)

    barrier = pltpu.get_barrier_semaphore()
    for d in range(1, row_dev):
        pl.semaphore_signal(barrier, inc=1, device_id={"row": (me_row + d) % row_dev})
    for d in range(1, col_dev):
        pl.semaphore_signal(barrier, inc=1, device_id={"col": (me_col + d) % col_dev})

    def span(q):
        return pl.ds(bounds[q], bounds[q + 1] - bounds[q])

    def block_rows(owner, q):
        return pl.ds(pl.multiple_of(owner * rows + bounds[q], 16), bounds[q + 1] - bounds[q])

    def load(q):
        return pltpu.make_async_copy(v_ref.at[span(q)], loaded.at[span(q)], load_sem.at[q])

    def remote(src, dst, send, recv, device):
        return pltpu.make_async_remote_copy(
            src_ref=src, dst_ref=dst, send_sem=send, recv_sem=recv, device_id=device
        )

    def drain(ref, sem):
        pltpu.make_async_copy(ref, ref, sem).wait()

    def line(zi, kind, q, to_end):
        part = row_panel.at[zi * CORES + core, span(q)]
        return remote(
            part, part, sent.at[to_end], line_recv.at[kind, q],
            {"col": outward if to_end else inward},
        )

    def pair(zi, q, slot):
        part = row_panel.at[zi * CORES + core, span(q)]
        return remote(
            part, part, sent.at[2], pair_recv.at[slot], {"col": z * CORES + 1 - core}
        )

    def ring(owner, q, to_right, last):
        part = col_panel.at[block_rows(owner, q)]
        return remote(
            part, part, sent.at[3], ring_recv.at[last, q],
            {"row": ring_device(1 if to_right else -1)},
        )

    def far_ring(q, to_right):
        return remote(
            row_panel.at[end * CORES + core, span(q)], far.at[block_rows(me_row, q)],
            sent.at[4], far_recv.at[q // 2], {"row": ring_device(1 if to_right else -1)},
        )

    def far_own(q):
        return pltpu.make_async_copy(
            row_panel.at[end * CORES + core, span(q)], far.at[block_rows(me_row, q)], small.at[7]
        )

    def far_line(q):
        part = block_rows(opposite, q)
        return remote(
            col_panel.at[part], far.at[part], sent.at[1], far_recv.at[2 + q // 2], {"col": inward}
        )

    def row_sum_copy(d):
        return remote(
            row_sums.at[0], row_sums.at[d], sent.at[5], small.at[0],
            {"row": (me_row + d) % row_dev},
        )

    def stat_copy(d):
        return remote(
            stats.at[0], stats.at[d], sent.at[6], small.at[1], {"col": (me_col + d) % col_dev}
        )

    def sum_copy(d):
        return remote(
            sums.at[0], sums.at[d], sent.at[7], small.at[2], {"row": (me_row + d) % row_dev}
        )

    def ahead_sum_copy(d):
        return remote(
            total_sums.at[0], ahead_sums.at[d], sent.at[8], small.at[3],
            {"row": (me_row + d) % row_dev, "col": outward},
        )

    def total_copy():
        return remote(
            total_sums.at[0], total_sums.at[1], sent.at[8], small.at[3], {"col": inward}
        )

    def note_copy():
        return remote(notes.at[0], notes.at[1], sent.at[9], small.at[4], {"col": inward})

    def early_copy():
        return remote(
            ahead.at[pl.ds(0, split)], acc.at[pl.ds(base, split)],
            sent.at[9], small.at[5], {"col": outward},
        )

    def done_copy():
        return remote(
            done, out_ref.at[pl.ds(base + split, rows - base - split)],
            sent.at[10], small.at[6], {"col": outward},
        )

    def own_ring(q):
        for to_right in (1, 0):
            ring(me_row, q, to_right, 0).start()

    def ring_wait(q):
        drain(col_panel.at[pl.ds(0, 2 * (bounds[q + 1] - bounds[q]))], ring_recv.at[0, q])

    def ring_relay(q, to_right):
        ring(ring_device(-1 if to_right else 1), q, to_right, 1).start()

    def ring_last(q):
        drain(col_panel.at[pl.ds(0, bounds[q + 1] - bounds[q])], ring_recv.at[1, q])

    def pair_slot(at_end, kind, q):
        if at_end:
            return 0 if kind == 0 else 2 * q + kind
        return 0 if q in raw else 1 + (kind == 2)

    def first_sends(q):
        @pl.when(is_end)
        def _():
            line(end, 0, q, 0).start()
            if q < 2:
                own_ring(q)
            if q in raw:
                pair(end, q, pair_slot(True, 0, q)).start()

        @pl.when(is_near)
        def _():
            if q < 2:
                line(near, 1, q, 0).start()
                own_ring(q)
            if q in raw:
                line(near, 0, q, 1).start()
            pair(near, q, pair_slot(False, 0, q)).start()

    for q in range(chunks):
        load(q).start()

    stored = tile_ref[...].astype(jnp.float32)
    kept = keep_ref[...].astype(jnp.float32)
    tile_sums = [jnp.zeros((1, TB), jnp.float32) for _ in range(cols // TB)]

    def mask(q):
        load(q).wait()
        for lo, hi in cut_rows(bounds[q], bounds[q + 1]):
            for b in range(cols // TB):
                r, c = slice(lo, hi), slice(b * TB, (b + 1) * TB)
                scale = jnp.broadcast_to(stored[b : b + 1, lo // TB : lo // TB + 1], (hi - lo, TB))
                tile = loaded[r, c].astype(jnp.float32) * scale
                tile_sums[b] += jnp.sum(tile, axis=0, keepdims=True)
                tile = tile.astype(jnp.bfloat16)
                row_panel[me_col, r, c] = tile
                col_panel[pl.ds(pl.multiple_of(me_row * rows + lo, 16), hi - lo), c] = tile

    mask(0)
    mask(1)
    pl.semaphore_wait(barrier, row_dev + col_dev - 2)
    first_sends(0)
    mask(2)
    first_sends(1)
    mask(3)
    row_sums[0] = jnp.concatenate(tile_sums, axis=1)
    first_sends(2)
    for d in range(1, row_dev):
        row_sum_copy(d).start()
    first_sends(3)

    def send_stats():
        drain(row_sums.at[pl.ds(1, row_dev - 1)], small.at[0])
        total = row_sums[0]
        for d in range(1, row_dev):
            total += row_sums[d]
        stats[0] = total
        for d in range(1, col_dev):
            stat_copy(d).start()

    def wait_stats():
        drain(stats.at[pl.ds(1, col_dev - 1)], small.at[1])

    def inner(owner, lane):
        return pl.ds(pl.multiple_of((owner * CORES + lane) * cols, cols), cols)

    def product_sums(owners, lanes=range(CORES)):
        total = jnp.zeros((1, cols), jnp.float32)
        for owner in owners:
            for lane in lanes:
                rest = stats[(me_col - owner * CORES - lane + col_dev) % col_dev]
                terms = []
                for _ in range(3):
                    term = rest.astype(jnp.bfloat16).astype(jnp.float32)
                    rest = rest - term
                    terms.append(jnp.broadcast_to(term, (8, cols)))
                spread = jnp.dot(
                    jnp.concatenate(terms, axis=0).astype(jnp.bfloat16),
                    col_panel[inner(owner, lane)], preferred_element_type=jnp.float32,
                )
                total += spread[16:17] + spread[8:9] + spread[0:1]
        return total

    def cuts(total):
        return 0.125 * thr_ref[...].astype(jnp.float32) * (total / order)

    def product(zis, q, lanes=range(CORES), panel=col_panel):
        total = None
        for zi in zis:
            for lane in lanes:
                term = jnp.dot(
                    row_panel[zi * CORES + lane, span(q)], panel[inner(zi, lane)],
                    preferred_element_type=jnp.float32,
                )
                total = term if total is None else total + term
        return total

    def prune(q, cut):
        parts = []
        for b in range(cols // TB):
            c = slice(b * TB, (b + 1) * TB)
            part = jnp.zeros((1, TB), jnp.float32)
            for lo, hi in cut_rows(bounds[q], bounds[q + 1]):
                keep = jnp.broadcast_to(kept[b : b + 1, lo // TB : lo // TB + 1], (hi - lo, TB))
                pruned = jnp.maximum(acc[lo:hi, c] - cut[:, c], 0.0) * keep
                acc[lo:hi, c] = pruned
                part += jnp.sum(pruned, axis=0, keepdims=True)
            parts.append(part)
        return jnp.concatenate(parts, axis=1)

    def normal(total):
        return 1.0 / jnp.maximum(total / order, 0.1)

    def all_sums():
        drain(sums.at[pl.ds(1, row_dev - 1)], small.at[2])
        part = sums[0]
        for d in range(1, row_dev):
            part += sums[d]
        return part

    @pl.when(is_end)
    def _():
        def arrive(kind, q):
            zi = (near, over, other)[kind]
            drain(row_panel.at[0, span(q)], line_recv.at[kind, q])
            pair(zi, q, pair_slot(True, kind, q)).start()

        def met(kind, q):
            drain(row_panel.at[0, span(q)], pair_recv.at[pair_slot(True, kind, q)])

        ring_wait(0)
        ring_relay(0, 1)
        own_ring(2)
        ring_wait(1)
        ring_relay(1, 0)
        own_ring(3)
        send_stats()
        arrive(0, 0)
        arrive(0, 1)
        ring_last(0)
        far_line(0).start()
        ring_wait(2)
        ring_relay(2, 1)
        arrive(0, 2)
        ring_last(1)
        far_line(1).start()
        ring_wait(3)
        ring_relay(3, 0)
        arrive(1, 0)
        arrive(1, 1)
        ring_last(2)
        far_line(2).start()
        ring_last(3)
        far_line(3).start()
        arrive(2, 0)
        wait_stats()
        cut = cuts(product_sums(range(chips)))
        note = [cut]
        for t in range(base // TB, base // TB + 7):
            t = min(t, rows // TB - 1)
            line_of = [
                jnp.broadcast_to(kept[b : b + 1, t : t + 1], (1, TB)) for b in range(cols // TB)
            ]
            note.append(jnp.concatenate(line_of, axis=1))
        notes[0] = jnp.concatenate(note, axis=0)
        drain(row_panel.at[pl.ds(0, 2), pl.ds(0, base)], pair_recv.at[0])
        acc[span(2)] = product((end, near), 2)
        note_copy().start()
        met(1, 0)
        met(1, 1)
        acc[span(1)] = product((end, near, over), 1)
        met(2, 0)
        acc[span(0)] = product((end, near, over, other), 0)
        part = prune(0, cut)
        arrive(1, 2)
        arrive(2, 1)
        met(1, 2)
        acc[span(2)] += product((over,), 2)
        met(2, 1)
        acc[span(1)] += product((other,), 1)
        part += prune(1, cut)
        arrive(2, 2)
        met(2, 2)
        acc[span(2)] += product((other,), 2)
        part += prune(2, cut)
        sums[0] = part
        for d in range(1, row_dev):
            sum_copy(d).start()
        part = all_sums()
        drain(ahead_sums, small.at[3])
        for d in range(row_dev):
            part += ahead_sums[d]
        total_sums[0] = part
        total_copy().start()
        scale = normal(part)
        out_ref[:base] = (acc[:base] * scale).astype(jnp.bfloat16)
        drain(ahead.at[pl.ds(0, split)], small.at[5])
        out_ref[base : base + split] = (acc[base : base + split] * scale).astype(jnp.bfloat16)
        drain(done, small.at[6])
        drain(row_panel.at[0], sent.at[0])
        drain(col_panel.at[pl.ds(0, rows)], sent.at[1])
        drain(row_panel.at[pl.ds(0, chips), pl.ds(0, base)], sent.at[2])
        drain(notes.at[0], sent.at[9])
        drain(total_sums.at[0], sent.at[8])

    @pl.when(is_near)
    def _():
        def arrive(kind, q, relay):
            zi = (end, over, other)[kind]
            drain(row_panel.at[0, span(q)], line_recv.at[kind, q])
            if relay is not None:
                line(zi, 2 if kind == 0 else kind, q, relay).start()
            pair(zi, q, pair_slot(False, kind, q)).start()

        def from_end(q):
            arrive(0, q, 0)
            if q % 2 == 0:
                line(near, 1, 2 + q // 2, 0).start()
            for to_right in (1, 0):
                far_ring(q, to_right).start()
            far_own(q).start()
            if q < 2:
                own_ring(q + 2)

        def from_over(kind, q):
            arrive(kind, q, 1 if q in raw else None)

        beside = (me_row, ring_device(1), ring_device(-1))
        from_end(0)
        from_over(1, 0)
        from_end(1)
        from_over(1, 1)
        send_stats()
        from_end(2)
        from_over(2, 0)
        from_end(3)
        ring_wait(0)
        ring_relay(0, 1)
        ring_wait(1)
        ring_relay(1, 1)
        from_over(1, 2)
        ring_wait(2)
        ring_relay(2, 0)
        from_over(2, 1)
        ring_wait(3)
        ring_relay(3, 0)
        from_over(2, 2)
        drain(row_panel.at[pl.ds(0, chips), pl.ds(0, base)], pair_recv.at[0])
        for q in raw:
            acc[span(q)] = product(beside, q)
        from_over(1, 3)
        drain(row_panel.at[pl.ds(0, 3), span(ahead_of)], pair_recv.at[1])
        drain(far.at[pl.ds(0, rows)], small.at[7])
        drain(far.at[pl.ds(0, 2 * bounds[2])], far_recv.at[0])
        drain(far.at[pl.ds(0, bounds[2])], far_recv.at[2])
        ahead[...] = product((end, near, over), ahead_of, (0,), far)
        from_over(2, 3)
        drain(far.at[pl.ds(0, 2 * (rows - bounds[2]))], far_recv.at[1])
        drain(far.at[pl.ds(0, rows - bounds[2])], far_recv.at[3])
        ahead[...] += product((end, near, over), ahead_of, (1,), far)
        drain(row_panel.at[0, span(ahead_of)], pair_recv.at[2])
        ahead[...] += product((other,), ahead_of, range(CORES), far)
        drain(notes.at[1], small.at[4])
        parts = jnp.zeros((1, cols), jnp.float32)
        for lo, hi in cut_rows(base, rows):
            tile = lo // TB - base // TB + 1
            pruned = jnp.maximum(ahead[lo - base : hi - base] - notes[1, 0:1], 0.0)
            pruned *= notes[1, tile : tile + 1]
            ahead[lo - base : hi - base] = pruned
            parts += jnp.sum(pruned, axis=0, keepdims=True)
        total_sums[0] = parts
        for d in range(row_dev):
            ahead_sum_copy(d).start()
        early_copy().start()
        acc[span(ahead_of)] = product(beside, ahead_of)
        wait_stats()
        head = product_sums(beside)
        drain(total_sums.at[1], small.at[3])
        scale = normal(total_sums[1])
        done[...] = (ahead[split:] * scale).astype(jnp.bfloat16)
        done_copy().start()
        ring_last(0)
        ring_last(1)
        for q in range(chunks):
            acc[span(q)] += product((opposite,), q, (0,))
        head += product_sums((opposite,), (0,))
        ring_last(2)
        ring_last(3)
        cut = cuts(head + product_sums((opposite,), (1,)))
        part = jnp.zeros((1, cols), jnp.float32)
        for q in range(chunks):
            acc[span(q)] += product((opposite,), q, (1,))
            part += prune(q, cut)
        sums[0] = part
        for d in range(1, row_dev):
            sum_copy(d).start()
        out_ref[...] = (acc[...] * normal(all_sums())).astype(jnp.bfloat16)
        drain(row_panel.at[pl.ds(0, 2)], sent.at[0])
        drain(row_panel.at[pl.ds(0, 3), pl.ds(0, base)], sent.at[1])
        drain(row_panel.at[pl.ds(0, chips)], sent.at[2])
        drain(far.at[pl.ds(0, 2 * rows)], sent.at[4])
        drain(ahead_sums, sent.at[8])
        drain(ahead.at[pl.ds(0, split)], sent.at[9])
        drain(done, sent.at[10])

    drain(col_panel.at[pl.ds(0, 3 * rows)], sent.at[3])
    drain(row_sums.at[pl.ds(1, row_dev - 1)], sent.at[5])
    drain(stats.at[pl.ds(1, col_dev - 1)], sent.at[6])
    drain(sums.at[pl.ds(1, row_dev - 1)], sent.at[7])


def near_call(values, tile_mask, keep_mask, thr_index, *, row_dev, col_dev, width):
    rows, cols = values.shape
    base = rows * 11 // 16 // 16 * 16
    split = (rows - base) * 2 // 5 // 16 * 16
    bounds = (0, cols // 32 * 16, cols, base, rows)
    chunks = len(bounds) - 1
    dma = pltpu.SemaphoreType.DMA
    vmem = pl.BlockSpec(memory_space=pltpu.VMEM)
    return pl.pallas_call(
        functools.partial(near_kernel, width, bounds, split, rows * row_dev),
        out_shape=pltpu.VMEM((rows, cols), jnp.bfloat16),
        in_specs=[pl.BlockSpec(memory_space=pl.ANY)] + [vmem] * 3,
        out_specs=vmem,
        scratch_shapes=[
            pltpu.VMEM((rows, cols), jnp.float32),
            pltpu.VMEM((col_dev, rows, cols), jnp.bfloat16),
            pltpu.VMEM((row_dev * rows, cols), jnp.bfloat16),
            pltpu.VMEM((row_dev * rows, cols), jnp.bfloat16),
            pltpu.VMEM((rows - base - split, cols), jnp.bfloat16),
            pltpu.VMEM((rows - base, cols), jnp.float32),
            pltpu.VMEM((row_dev, 1, cols), jnp.float32),
            pltpu.VMEM((col_dev, 1, cols), jnp.float32),
            pltpu.VMEM((row_dev, 1, cols), jnp.float32),
            pltpu.VMEM((row_dev, 1, cols), jnp.float32),
            pltpu.VMEM((2, 1, cols), jnp.float32),
            pltpu.VMEM((2, 8, cols), jnp.float32),
            pltpu.VMEM((rows, cols), jnp.bfloat16),
            dma((11,)), dma((8,)),
            dma((3, chunks)), dma((7,)), dma((2, chunks)), dma((4,)), dma((chunks,)),
        ],
        compiler_params=pltpu.CompilerParams(
            collective_id=0, has_side_effects=True,
            vmem_limit_bytes=63 * 2**20 - 2 * rows * cols,
        ),
    )(values, tile_mask.T, keep_mask.T, thr_index.reshape(1, cols))


def on_device(values, tile_mask, keep_mask, thr_index, *, row_dev, col_dev):
    rows, cols = values.shape
    width = max(w for w in range(1, row_dev + 1) if row_dev % w == 0 and w * w <= row_dev)
    chips = col_dev // CORES
    if chips == 4 and row_dev == 4 and rows == CORES * cols:
        return near_call(
            values, tile_mask, keep_mask, thr_index, row_dev=row_dev, col_dev=col_dev, width=width
        )
    dma = pltpu.SemaphoreType.DMA
    vmem = pl.BlockSpec(memory_space=pltpu.VMEM)
    pruned, scale = pl.pallas_call(
        functools.partial(kernel, row_dev, col_dev, width, CHUNKS, rows * row_dev),
        out_shape=(
            pltpu.VMEM((rows, cols), jnp.float32),
            jax.ShapeDtypeStruct((1, cols), jnp.float32),
        ),
        in_specs=[pl.BlockSpec(memory_space=pl.ANY)] + [vmem] * 3,
        out_specs=(vmem, vmem),
        scratch_shapes=[
            pltpu.VMEM((col_dev, rows, cols), jnp.bfloat16),
            pltpu.VMEM((row_dev * rows, cols), jnp.bfloat16),
            pltpu.VMEM((row_dev, 1, cols), jnp.float32),
            pltpu.VMEM((col_dev, 1, cols), jnp.float32),
            dma((2, chips, CHUNKS)),
            dma((chips, CHUNKS)),
            dma((chips, CHUNKS)),
            dma((chips, CHUNKS)),
            dma((2, row_dev, CHUNKS)),
            dma((row_dev, CHUNKS)),
            dma((row_dev,)),
            dma((row_dev,)),
            dma((col_dev,)),
            dma((col_dev,)),
            pltpu.VMEM((rows, cols), jnp.bfloat16),
            dma((CHUNKS,)),
            pltpu.SemaphoreType.REGULAR((2,)),
        ],
        compiler_params=pltpu.CompilerParams(
            collective_id=0, has_side_effects=True,
            vmem_limit_bytes=63 * 2**20 - 4 * rows * cols + 2**19,
        ),
    )(values, tile_mask.T, keep_mask.T, thr_index.reshape(1, cols))
    return (pruned * scale).astype(jnp.bfloat16)


def solution(mesh):
    return jax.shard_map(
        functools.partial(on_device, row_dev=mesh.shape["row"], col_dev=mesh.shape["col"]),
        mesh=mesh,
        in_specs=(P("row", "col"), P("row", "col"), P("row", "col"), P("col")),
        out_specs=P("row", "col"),
        check_vma=False,
    )
```

```python
import functools

import jax
import jax.numpy as jnp
from jax import lax
from jax.experimental import pallas as pl
from jax.experimental.pallas import tpu as pltpu
from jax.sharding import PartitionSpec as P

TB = 128
CORES = 2
CHUNKS = 4


def snake(index, width):
    line, spot = index // width, index % width
    return line * width + spot + (line % 2) * (width - 1 - 2 * spot)


def kernel(
    row_dev, col_dev, width, chunks, order,
    v_ref, tile_ref, keep_ref, thr_ref, acc, totals_ref,
    row_panel, col_panel, sums, stats,
    line_send, line_recv, pair_send, pair_recv, ring_send, ring_recv,
    sum_send, sum_recv, stat_send, stat_recv, loaded, load_sem, token,
):
    rows, cols = v_ref.shape
    step_rows = rows // chunks
    chips = col_dev // CORES
    half = row_dev // 2
    me_row, me_col = lax.axis_index("row"), lax.axis_index("col")
    z, core = me_col // CORES, me_col % CORES
    pos = snake(me_row, width)

    def ring_device(offset):
        return snake((pos + offset + row_dev) % row_dev, width)

    barrier = pltpu.get_barrier_semaphore()
    pl.semaphore_signal(barrier, inc=1, device_id={"col": z * CORES + 1 - core})
    peers = 1 + (z > 0).astype(jnp.int32) + (z < chips - 1).astype(jnp.int32)
    for offset in ((1, -1) if row_dev > 2 else (1,) * half):
        pl.semaphore_signal(barrier, inc=1, device_id={"row": ring_device(offset)})
        peers += 1

    @pl.when(z > 0)
    def _():
        pl.semaphore_signal(barrier, inc=1, device_id={"col": me_col - CORES})

    @pl.when(z < chips - 1)
    def _():
        pl.semaphore_signal(barrier, inc=1, device_id={"col": me_col + CORES})

    def load(q):
        spot = pl.ds(q * step_rows, step_rows)
        return pltpu.make_async_copy(v_ref.at[spot], loaded.at[spot], load_sem.at[q])

    for q in range(chunks):
        load(q).start()

    stored = tile_ref[...].astype(jnp.float32)
    kept = keep_ref[...].astype(jnp.float32)
    height = min(step_rows, TB)
    for lo in range(0, rows, height):
        if lo % step_rows == 0:
            load(lo // step_rows).wait()
        for b in range(cols // TB):
            r, c = slice(lo, lo + height), slice(b * TB, (b + 1) * TB)
            scale = jnp.broadcast_to(stored[b : b + 1, lo // TB : lo // TB + 1], (height, TB))
            tile = (loaded[r, c].astype(jnp.float32) * scale).astype(jnp.bfloat16)
            row_panel[me_col, r, c] = tile
            col_panel[pl.ds(pl.multiple_of(me_row * rows + lo, height), height), c] = tile

    pl.semaphore_wait(barrier, peers)

    def row_part(block, q):
        return row_panel.at[block, pl.ds(q * step_rows, step_rows)]

    def line_copy(zi, q, to_right):
        part = row_part(zi * CORES + core, q)
        return pltpu.make_async_remote_copy(
            src_ref=part, dst_ref=part,
            send_sem=line_send.at[to_right, zi, q], recv_sem=line_recv.at[zi, q],
            device_id={"col": me_col + (CORES if to_right else -CORES)},
        )

    def pair_copy(zi, q, lane):
        part = row_part(zi * CORES + lane, q)
        return pltpu.make_async_remote_copy(
            src_ref=part, dst_ref=part,
            send_sem=pair_send.at[zi, q], recv_sem=pair_recv.at[zi, q],
            device_id={"col": z * CORES + 1 - core},
        )

    def ring_copy(owner, q, to_right):
        start = pl.multiple_of(owner * rows + q * step_rows, step_rows)
        part = col_panel.at[pl.ds(start, step_rows)]
        return pltpu.make_async_remote_copy(
            src_ref=part, dst_ref=part,
            send_sem=ring_send.at[to_right, owner, q], recv_sem=ring_recv.at[owner, q],
            device_id={"row": ring_device(1 if to_right else -1)},
        )

    def on_ring(d, q, to_right):
        if d < half:
            return True
        return d == half and (q < chunks // 2) == bool(to_right)

    def relay(zi, q, to_right, wait):
        if wait:
            line_copy(zi, q, to_right).wait_recv()
        go = (z < chips - 1) if to_right else (z > 0)

        @pl.when(go)
        def _():
            line_copy(zi, q, to_right).start()

    for q in range(chunks):
        for to_right in (1, 0):
            relay(z, q, to_right, False)
            if on_ring(1, q, to_right):
                ring_copy(me_row, q, to_right).start()
        pair_copy(z, q, core).start()

    for to_right in (1, 0):
        first, end = (0, chips - 1) if to_right else (chips - 1, 0)

        @pl.when(z != first)
        def _():
            pl.semaphore_wait(token.at[to_right], 1)

        @pl.when(z != end)
        def _():
            pl.semaphore_signal(
                token.at[to_right], inc=1,
                device_id={"col": me_col + (CORES if to_right else -CORES)},
            )

    def line_step(t, q):
        for to_right in (1, 0):
            valid = (z >= t) if to_right else (z + t < chips)
            zi = z - t if to_right else z + t
            if t < chips:
                @pl.when(valid)
                def _():
                    relay(zi, q, to_right, True)
                    pair_copy(zi, q, core).start()

    def ring_step(t, q):
        for to_right in (1, 0):
            if on_ring(t, q, to_right):
                owner = ring_device(-t if to_right else t)
                ring_copy(owner, q, to_right).wait_recv()
                if on_ring(t + 1, q, to_right):
                    ring_copy(owner, q, to_right).start()

    def stat_copy(d):
        return pltpu.make_async_remote_copy(
            src_ref=stats.at[0], dst_ref=stats.at[d],
            send_sem=stat_send.at[d], recv_sem=stat_recv.at[d],
            device_id={"col": (me_col + d) % col_dev},
        )

    def send_stats():
        total = jnp.zeros((1, cols), jnp.float32)
        for i in range(row_dev):
            block = col_panel[i * rows : (i + 1) * rows].astype(jnp.float32)
            total += jnp.sum(block, axis=0, keepdims=True)
        stats[0] = total
        for d in range(1, col_dev):
            stat_copy(d).start()

    def product_sums():
        total = jnp.zeros((1, cols), jnp.float32)
        for d in range(col_dev):
            if d:
                stat_copy(d).wait()
            block = (me_col - d + col_dev) % col_dev
            inner = pl.ds(pl.multiple_of(block * cols, cols), cols)
            rest, terms = stats[d], []
            for _ in range(3):
                term = rest.astype(jnp.bfloat16).astype(jnp.float32)
                rest = rest - term
                terms.append(jnp.broadcast_to(term, (8, cols)))
            spread = jnp.dot(
                jnp.concatenate(terms, axis=0).astype(jnp.bfloat16), col_panel[inner],
                preferred_element_type=jnp.float32,
            )
            total += spread[16:17] + spread[8:9] + spread[0:1]
        return total

    def compute(zi, q, first=False):
        spot = pl.ds(pl.multiple_of(q * step_rows, step_rows), step_rows)
        total = None
        for lane in range(CORES):
            block = zi * CORES + lane
            inner = pl.ds(pl.multiple_of(block * cols, cols), cols)
            term = jnp.dot(
                row_panel[block, spot], col_panel[inner], preferred_element_type=jnp.float32
            )
            total = term if total is None else total + term
        if first:
            acc[spot] = total
        else:
            acc[spot] += total

    def take(zi, q, first=False):
        pair_copy(zi, q, 1 - core).wait_recv()
        compute(zi, q, first)

    def sides(t):
        return ((z >= t, z - t), (z + t < chips, z + t))

    def bulk(upto):
        @pl.loop(0, chunks)
        def _(q):
            take(z, q, True)
            for t in range(1, min(upto, chips - 1) + 1):
                for valid, zi in sides(t):
                    @pl.when(valid)
                    def _():
                        take(zi, q)

    def prune(q, cut):
        parts = []
        for b in range(cols // TB):
            c = slice(b * TB, (b + 1) * TB)
            part = jnp.zeros((1, TB), jnp.float32)
            for lo in range(q * step_rows, (q + 1) * step_rows, min(step_rows, TB)):
                r = slice(lo, lo + min(step_rows, TB))
                keep = jnp.broadcast_to(kept[b : b + 1, lo // TB : lo // TB + 1], (r.stop - lo, TB))
                pruned = jnp.maximum(acc[r, c] - cut[:, c], 0.0) * keep
                acc[r, c] = pruned
                part += jnp.sum(pruned, axis=0, keepdims=True)
            parts.append(part)
        return jnp.concatenate(parts, axis=1)

    def cuts():
        return 0.125 * thr_ref[...].astype(jnp.float32) * (product_sums() / order)

    part = jnp.zeros((1, cols), jnp.float32)
    last = max(chips - 1, half)
    if half == 0:
        send_stats()
        bulk(0)
    for t in range(1, last + 1):
        if t == half:
            for q in range(chunks):
                ring_step(t, q)
            send_stats()
            for q in range(chunks):
                line_step(t, q)
            bulk(t)
        else:
            if t == last and t > half:
                cut = cuts()
            for q in range(chunks):
                line_step(t, q)
                if t < half:
                    ring_step(t, q)
                else:
                    for valid, zi in sides(t):
                        @pl.when(valid)
                        def _():
                            take(zi, q)
                    if t == last:
                        part += prune(q, cut)
    if last <= half:
        cut = cuts()
        for q in range(chunks):
            part += prune(q, cut)

    sums[0] = part

    def sum_copy(d):
        return pltpu.make_async_remote_copy(
            src_ref=sums.at[0], dst_ref=sums.at[d],
            send_sem=sum_send.at[d], recv_sem=sum_recv.at[d],
            device_id={"row": (me_row + d) % row_dev},
        )

    for d in range(1, row_dev):
        sum_copy(d).start()
    for d in range(1, row_dev):
        sum_copy(d).wait()
        part += sums[d]
    totals_ref[...] = 1.0 / jnp.maximum(part / order, 0.1)

    for q in range(chunks):
        for zi in range(chips):
            pair_copy(zi, q, core).wait_send()

            @pl.when((z < chips - 1) & (z >= zi))
            def _():
                line_copy(zi, q, 1).wait_send()

            @pl.when((z > 0) & (z <= zi))
            def _():
                line_copy(zi, q, 0).wait_send()
        for d in range(0, half):
            for to_right in (1, 0):
                if on_ring(d + 1, q, to_right):
                    owner = ring_device(-d if to_right else d)
                    ring_copy(owner, q, to_right).wait_send()


def cut_rows(lo, hi):
    while lo < hi:
        stop = min(hi, (lo // TB + 1) * TB)
        yield lo, stop
        lo = stop


def near_kernel(
    width, bounds, split, order,
    v_ref, tile_hbm, keep_hbm, thr_hbm, out_ref, acc, tile_ref, keep_ref, thr_ref,
    row_panel, col_panel, far, done, ahead, detour,
    row_sums, stats, sums, ahead_sums, total_sums, notes, loaded,
    sent, small, line_recv, pair_recv, ring_recv, far_recv, load_sem, token,
):
    rows, cols = v_ref.shape
    row_dev, col_dev, chips = row_sums.shape[0], stats.shape[0], stats.shape[0] // CORES
    chunks = len(bounds) - 1
    ahead_of = chunks - 1
    base = bounds[ahead_of]
    raw = range(ahead_of)
    me_row, me_col = lax.axis_index("row"), lax.axis_index("col")
    z, core = me_col // CORES, me_col % CORES
    pos = snake(me_row, width)
    on_right = z >= chips // 2
    end = jnp.where(on_right, chips - 1, 0)
    out = jnp.where(on_right, 1, -1)
    near, over, other = end - out, end - 2 * out, end - 3 * out
    is_end = z == end
    is_near = z == near
    inward, outward = me_col - CORES * out, me_col + CORES * out

    def ring_device(offset):
        return snake((pos + offset + row_dev) % row_dev, width)

    opposite = ring_device(2)

    barrier = pltpu.get_barrier_semaphore()
    for d in range(1, row_dev):
        pl.semaphore_signal(barrier, inc=1, device_id={"row": (me_row + d) % row_dev})
    pl.semaphore_signal(barrier, inc=1, device_id={"col": z * CORES + 1 - core})
    pl.semaphore_signal(barrier, inc=1, device_id={"col": inward})

    @pl.when(is_near)
    def _():
        pl.semaphore_signal(barrier, inc=1, device_id={"col": outward})


    def span(q):
        return pl.ds(bounds[q], bounds[q + 1] - bounds[q])

    def block_rows(owner, q):
        return pl.ds(pl.multiple_of(owner * rows + bounds[q], 16), bounds[q + 1] - bounds[q])

    def load(q):
        return pltpu.make_async_copy(v_ref.at[span(q)], loaded.at[span(q)], load_sem.at[q])

    def remote(src, dst, send, recv, device):
        return pltpu.make_async_remote_copy(
            src_ref=src, dst_ref=dst, send_sem=send, recv_sem=recv, device_id=device
        )

    def drain(ref, sem):
        pltpu.make_async_copy(ref, ref, sem).wait()

    def line(zi, kind, q, to_end):
        part = row_panel.at[zi * CORES + core, span(q)]
        return remote(
            part, part, sent.at[to_end], line_recv.at[kind, q],
            {"col": outward if to_end else inward},
        )

    def pair(zi, q, slot):
        part = row_panel.at[zi * CORES + core, span(q)]
        return remote(
            part, part, sent.at[2], pair_recv.at[slot], {"col": z * CORES + 1 - core}
        )

    def ring(owner, q, to_right, last):
        part = col_panel.at[block_rows(owner, q)]
        return remote(
            part, part, sent.at[3], ring_recv.at[last, q],
            {"row": ring_device(1 if to_right else -1)},
        )

    def far_ring(q, to_right):
        return remote(
            row_panel.at[end * CORES + core, span(q)], far.at[block_rows(me_row, q)],
            sent.at[4], far_recv.at[q // 2], {"row": ring_device(1 if to_right else -1)},
        )

    def far_own(q):
        return pltpu.make_async_copy(
            row_panel.at[end * CORES + core, span(q)], far.at[block_rows(me_row, q)], small.at[7]
        )

    def far_line(q):
        part = block_rows(opposite, q)
        return remote(
            col_panel.at[part], far.at[part], sent.at[1], far_recv.at[2 + q // 2], {"col": inward}
        )

    def detour_cross():
        return remote(
            row_panel.at[near * CORES + core, span(0)], detour, sent.at[4], small.at[8],
            {"row": opposite},
        )

    def detour_down():
        return remote(
            detour, col_panel.at[block_rows(opposite, 0)], sent.at[10], ring_recv.at[1, 0],
            {"col": inward},
        )

    def row_sum_copy(d):
        return remote(
            row_sums.at[0], row_sums.at[d], sent.at[5], small.at[0],
            {"row": (me_row + d) % row_dev},
        )

    def stat_copy(d):
        return remote(
            stats.at[0], stats.at[d], sent.at[6], small.at[1], {"col": (me_col + d) % col_dev}
        )

    def sum_copy(d):
        return remote(
            sums.at[0], sums.at[d], sent.at[7], small.at[2], {"row": (me_row + d) % row_dev}
        )

    def ahead_sum_copy(d):
        return remote(
            total_sums.at[0], ahead_sums.at[d], sent.at[8], small.at[3],
            {"row": (me_row + d) % row_dev, "col": outward},
        )

    def total_copy():
        return remote(
            total_sums.at[0], total_sums.at[1], sent.at[8], small.at[3], {"col": inward}
        )

    def note_copy():
        return remote(notes.at[0], notes.at[1], sent.at[9], small.at[4], {"col": inward})

    def early_copy():
        return remote(
            ahead.at[pl.ds(0, split)], acc.at[pl.ds(base, split)],
            sent.at[9], small.at[5], {"col": outward},
        )

    def done_copy():
        return remote(
            done, out_ref.at[pl.ds(base + split, rows - base - split)],
            sent.at[10], small.at[6], {"col": outward},
        )

    def own_ring(q):
        for to_right in (1, 0):
            ring(me_row, q, to_right, 0).start()

    def ring_wait(q):
        drain(col_panel.at[pl.ds(0, 2 * (bounds[q + 1] - bounds[q]))], ring_recv.at[0, q])

    def ring_relay_both(q):
        middle = (bounds[q] + bounds[q + 1]) // 32 * 16
        for to_right in (1, 0):
            lo, hi = (bounds[q], middle) if to_right else (middle, bounds[q + 1])
            owner = ring_device(-1 if to_right else 1)
            part = col_panel.at[pl.ds(pl.multiple_of(owner * rows + lo, 16), hi - lo)]
            remote(
                part, part, sent.at[3], ring_recv.at[1, q],
                {"row": ring_device(1 if to_right else -1)},
            ).start()

    def ring_relay(q, to_right):
        ring(ring_device(-1 if to_right else 1), q, to_right, 1).start()

    def ring_last(q):
        drain(col_panel.at[pl.ds(0, bounds[q + 1] - bounds[q])], ring_recv.at[1, q])

    def pair_slot(at_end, kind, q):
        if at_end:
            return 0 if kind == 0 else 2 * q + kind
        return 0 if q in raw else 1 + (kind == 2)

    def first_sends(q):
        @pl.when(is_end)
        def _():
            line(end, 0, q, 0).start()
            if q in (0, ahead_of):
                own_ring(q)
            if q in raw:
                pair(end, q, pair_slot(True, 0, q)).start()

        @pl.when(is_near)
        def _():
            if q < 2:
                line(near, 1, q, 0).start()
                own_ring(q)
            if q in raw:
                line(near, 0, q, 1).start()
            pair(near, q, pair_slot(False, 0, q)).start()

    tables = [
        pltpu.make_async_copy(src, dst, load_sem.at[chunks + i])
        for i, (src, dst) in enumerate(
            ((tile_hbm, tile_ref), (keep_hbm, keep_ref), (thr_hbm, thr_ref))
        )
    ]
    load(0).start()
    for table in tables:
        table.start()
    for q in range(1, chunks):
        load(q).start()
    for table in tables:
        table.wait()

    stored = tile_ref[...].astype(jnp.float32)
    kept = keep_ref[...].astype(jnp.float32)
    tile_sums = [jnp.zeros((1, TB), jnp.float32) for _ in range(cols // TB)]

    def mask(q):
        load(q).wait()
        for lo, hi in cut_rows(bounds[q], bounds[q + 1]):
            for b in range(cols // TB):
                r, c = slice(lo, hi), slice(b * TB, (b + 1) * TB)
                scale = jnp.broadcast_to(stored[b : b + 1, lo // TB : lo // TB + 1], (hi - lo, TB))
                tile = loaded[r, c].astype(jnp.float32) * scale
                tile_sums[b] += jnp.sum(tile, axis=0, keepdims=True)
                tile = tile.astype(jnp.bfloat16)
                row_panel[me_col, r, c] = tile
                col_panel[pl.ds(pl.multiple_of(me_row * rows + lo, 16), hi - lo), c] = tile

    mask(0)
    mask(1)
    pl.semaphore_wait(barrier, row_dev + 1 + is_near.astype(jnp.int32))

    @pl.when(is_end)
    def _():
        pl.semaphore_signal(token.at[0], inc=1, device_id={"col": inward})

    first_sends(0)
    mask(2)
    first_sends(1)
    mask(3)
    row_sums[0] = jnp.concatenate(tile_sums, axis=1)
    first_sends(2)
    for d in range(1, row_dev):
        row_sum_copy(d).start()
    first_sends(3)

    def send_stats():
        drain(row_sums.at[pl.ds(1, row_dev - 1)], small.at[0])
        total = row_sums[0]
        for d in range(1, row_dev):
            total += row_sums[d]
        stats[0] = total
        for d in range(1, col_dev):
            stat_copy(d).start()

    def wait_stats():
        drain(stats.at[pl.ds(1, col_dev - 1)], small.at[1])

    def inner(owner, lane):
        return pl.ds(pl.multiple_of((owner * CORES + lane) * cols, cols), cols)

    def product_sums(owners, lanes=range(CORES)):
        total = jnp.zeros((1, cols), jnp.float32)
        for owner in owners:
            for lane in lanes:
                rest = stats[(me_col - owner * CORES - lane + col_dev) % col_dev]
                terms = []
                for _ in range(3):
                    term = rest.astype(jnp.bfloat16).astype(jnp.float32)
                    rest = rest - term
                    terms.append(jnp.broadcast_to(term, (8, cols)))
                spread = jnp.dot(
                    jnp.concatenate(terms, axis=0).astype(jnp.bfloat16),
                    col_panel[inner(owner, lane)], preferred_element_type=jnp.float32,
                )
                total += spread[16:17] + spread[8:9] + spread[0:1]
        return total

    def cuts(total):
        return 0.125 * thr_ref[...].astype(jnp.float32) * (total / order)

    def product(zis, q, lanes=range(CORES), panel=col_panel):
        total = None
        for zi in zis:
            for lane in lanes:
                term = jnp.dot(
                    row_panel[zi * CORES + lane, span(q)], panel[inner(zi, lane)],
                    preferred_element_type=jnp.float32,
                )
                total = term if total is None else total + term
        return total

    def prune(q, cut):
        parts = []
        for b in range(cols // TB):
            c = slice(b * TB, (b + 1) * TB)
            part = jnp.zeros((1, TB), jnp.float32)
            for lo, hi in cut_rows(bounds[q], bounds[q + 1]):
                keep = jnp.broadcast_to(kept[b : b + 1, lo // TB : lo // TB + 1], (hi - lo, TB))
                pruned = jnp.maximum(acc[lo:hi, c] - cut[:, c], 0.0) * keep
                acc[lo:hi, c] = pruned
                part += jnp.sum(pruned, axis=0, keepdims=True)
            parts.append(part)
        return jnp.concatenate(parts, axis=1)

    def normal(total):
        return 1.0 / jnp.maximum(total / order, 0.1)

    def all_sums():
        drain(sums.at[pl.ds(1, row_dev - 1)], small.at[2])
        part = sums[0]
        for d in range(1, row_dev):
            part += sums[d]
        return part

    @pl.when(is_end)
    def _():
        def arrive(kind, q):
            zi = (near, over, other)[kind]
            drain(row_panel.at[0, span(q)], line_recv.at[kind, q])
            pair(zi, q, pair_slot(True, kind, q)).start()

        def met(kind, q):
            drain(row_panel.at[0, span(q)], pair_recv.at[pair_slot(True, kind, q)])

        ring_wait(0)
        ring_relay(0, 1)
        own_ring(1)
        arrive(0, 0)
        arrive(0, 1)
        ring_wait(3)
        ring_relay(3, 0)
        own_ring(2)
        arrive(0, 2)
        ring_last(0)
        far_line(0).start()
        pl.semaphore_wait(token.at[1], 1)
        send_stats()
        arrive(1, 0)
        ring_wait(1)
        ring_relay(1, 1)
        ring_last(3)
        far_line(3).start()
        arrive(1, 1)
        ring_wait(2)
        ring_relay(2, 0)
        detour_cross().start()
        ring_last(1)
        far_line(1).start()
        arrive(2, 0)
        ring_last(2)
        far_line(2).start()
        wait_stats()
        cut = cuts(product_sums(range(chips)))
        note = [cut]
        for t in range(base // TB, base // TB + 7):
            t = min(t, rows // TB - 1)
            line_of = [
                jnp.broadcast_to(kept[b : b + 1, t : t + 1], (1, TB)) for b in range(cols // TB)
            ]
            note.append(jnp.concatenate(line_of, axis=1))
        notes[0] = jnp.concatenate(note, axis=0)
        drain(row_panel.at[pl.ds(0, 2), pl.ds(0, base)], pair_recv.at[0])
        acc[span(2)] = product((end, near), 2)
        note_copy().start()
        met(1, 0)
        met(1, 1)
        acc[span(1)] = product((end, near, over), 1)
        met(2, 0)
        acc[span(0)] = product((end, near, over, other), 0)
        part = prune(0, cut)
        drain(detour, small.at[8])
        detour_down().start()
        arrive(1, 2)
        arrive(2, 1)
        met(1, 2)
        acc[span(2)] += product((over,), 2)
        met(2, 1)
        acc[span(1)] += product((other,), 1)
        part += prune(1, cut)
        arrive(2, 2)
        met(2, 2)
        acc[span(2)] += product((other,), 2)
        part += prune(2, cut)
        sums[0] = part
        for d in range(1, row_dev):
            sum_copy(d).start()
        part = all_sums()
        drain(ahead_sums, small.at[3])
        for d in range(row_dev):
            part += ahead_sums[d]
        total_sums[0] = part
        total_copy().start()
        scale = normal(part)
        out_ref[:base] = (acc[:base] * scale).astype(jnp.bfloat16)
        drain(ahead.at[pl.ds(0, split)], small.at[5])
        out_ref[base : base + split] = (acc[base : base + split] * scale).astype(jnp.bfloat16)
        drain(done, small.at[6])
        drain(row_panel.at[0], sent.at[0])
        drain(col_panel.at[pl.ds(0, rows)], sent.at[1])
        drain(row_panel.at[pl.ds(0, chips), pl.ds(0, base)], sent.at[2])
        drain(notes.at[0], sent.at[9])
        drain(total_sums.at[0], sent.at[8])
        drain(col_panel.at[pl.ds(0, 3 * rows)], sent.at[3])
        drain(detour, sent.at[4])
        drain(detour, sent.at[10])

    @pl.when(is_near)
    def _():
        def arrive(kind, q, relay):
            zi = (end, over, other)[kind]
            drain(row_panel.at[0, span(q)], line_recv.at[kind, q])
            if relay is not None:
                line(zi, 2 if kind == 0 else kind, q, relay).start()
            pair(zi, q, pair_slot(False, kind, q)).start()

        def from_end(q):
            arrive(0, q, 0)
            if q % 2 == 0:
                line(near, 1, 2 + q // 2, 0).start()
            for to_right in (1, 0):
                far_ring(q, to_right).start()
            far_own(q).start()
            if q < 2:
                own_ring(q + 2)

        def from_over(kind, q):
            arrive(kind, q, 1 if q in raw else None)

        beside = (me_row, ring_device(1), ring_device(-1))
        from_end(0)
        pl.semaphore_wait(token.at[0], 1)
        pl.semaphore_signal(token.at[1], inc=1, device_id={"col": inward})
        from_over(1, 0)
        from_end(1)
        from_over(1, 1)
        pl.semaphore_wait(token.at[1], 1)
        pl.semaphore_signal(token.at[1], inc=1, device_id={"col": outward})
        send_stats()
        from_end(2)
        from_over(2, 0)
        from_end(3)
        ring_wait(0)
        ring_wait(1)
        ring_relay(1, 1)
        from_over(1, 2)
        ring_wait(2)
        ring_relay_both(2)
        from_over(2, 1)
        ring_wait(3)
        ring_relay(3, 0)
        from_over(2, 2)
        drain(row_panel.at[pl.ds(0, chips), pl.ds(0, base)], pair_recv.at[0])
        for q in raw:
            acc[span(q)] = product(beside, q)
        from_over(1, 3)
        drain(row_panel.at[pl.ds(0, 3), span(ahead_of)], pair_recv.at[1])
        drain(far.at[pl.ds(0, rows)], small.at[7])
        drain(far.at[pl.ds(0, 2 * bounds[2])], far_recv.at[0])
        drain(far.at[pl.ds(0, bounds[2])], far_recv.at[2])
        ahead[...] = product((end, near, over), ahead_of, (0,), far)
        from_over(2, 3)
        drain(far.at[pl.ds(0, 2 * (rows - bounds[2]))], far_recv.at[1])
        drain(far.at[pl.ds(0, rows - bounds[2])], far_recv.at[3])
        ahead[...] += product((end, near, over), ahead_of, (1,), far)
        drain(row_panel.at[0, span(ahead_of)], pair_recv.at[2])
        ahead[...] += product((other,), ahead_of, range(CORES), far)
        drain(notes.at[1], small.at[4])
        parts = jnp.zeros((1, cols), jnp.float32)
        for lo, hi in cut_rows(base, rows):
            tile = lo // TB - base // TB + 1
            pruned = jnp.maximum(ahead[lo - base : hi - base] - notes[1, 0:1], 0.0)
            pruned *= notes[1, tile : tile + 1]
            ahead[lo - base : hi - base] = pruned
            parts += jnp.sum(pruned, axis=0, keepdims=True)
        total_sums[0] = parts
        for d in range(row_dev):
            ahead_sum_copy(d).start()
        early_copy().start()
        acc[span(ahead_of)] = product(beside, ahead_of)
        wait_stats()
        head = product_sums(beside)
        ring_last(1)
        ring_last(0)
        for q in range(chunks):
            acc[span(q)] += product((opposite,), q, (0,))
        head += product_sums((opposite,), (0,))
        drain(total_sums.at[1], small.at[3])
        scale = normal(total_sums[1])
        done[...] = (ahead[split:] * scale).astype(jnp.bfloat16)
        done_copy().start()
        ring_last(2)
        ring_last(3)
        cut = cuts(head + product_sums((opposite,), (1,)))
        part = jnp.zeros((1, cols), jnp.float32)
        for q in range(chunks):
            acc[span(q)] += product((opposite,), q, (1,))
            part += prune(q, cut)
        sums[0] = part
        for d in range(1, row_dev):
            sum_copy(d).start()
        out_ref[...] = (acc[...] * normal(all_sums())).astype(jnp.bfloat16)
        drain(row_panel.at[pl.ds(0, 2)], sent.at[0])
        drain(row_panel.at[pl.ds(0, 3), pl.ds(0, base)], sent.at[1])
        drain(row_panel.at[pl.ds(0, chips)], sent.at[2])
        drain(far.at[pl.ds(0, 2 * rows)], sent.at[4])
        drain(ahead_sums, sent.at[8])
        drain(ahead.at[pl.ds(0, split)], sent.at[9])
        drain(done, sent.at[10])
        drain(col_panel.at[pl.ds(0, 3 * rows - bounds[1])], sent.at[3])

    drain(row_sums.at[pl.ds(1, row_dev - 1)], sent.at[5])
    drain(stats.at[pl.ds(1, col_dev - 1)], sent.at[6])
    drain(sums.at[pl.ds(1, row_dev - 1)], sent.at[7])


def near_call(values, tile_mask, keep_mask, thr_index, *, row_dev, col_dev, width):
    rows, cols = values.shape
    base = rows * 45 // 64 // 16 * 16
    split = (rows - base) // 32 * 16
    bounds = (0, cols // 32 * 16, cols, base, rows)
    chunks = len(bounds) - 1
    dma = pltpu.SemaphoreType.DMA
    vmem = pl.BlockSpec(memory_space=pltpu.VMEM)
    return pl.pallas_call(
        functools.partial(near_kernel, width, bounds, split, rows * row_dev),
        out_shape=pltpu.VMEM((rows, cols), jnp.bfloat16),
        in_specs=[pl.BlockSpec(memory_space=pl.ANY)] * 4,
        out_specs=vmem,
        scratch_shapes=[
            pltpu.VMEM((rows, cols), jnp.float32),
            pltpu.VMEM(tile_mask.shape[::-1], jnp.int32),
            pltpu.VMEM(keep_mask.shape[::-1], jnp.int32),
            pltpu.VMEM((1, cols), jnp.int32),
            pltpu.VMEM((col_dev, rows, cols), jnp.bfloat16),
            pltpu.VMEM((row_dev * rows, cols), jnp.bfloat16),
            pltpu.VMEM((row_dev * rows, cols), jnp.bfloat16),
            pltpu.VMEM((rows - base - split, cols), jnp.bfloat16),
            pltpu.VMEM((rows - base, cols), jnp.float32),
            pltpu.VMEM((bounds[1], cols), jnp.bfloat16),
            pltpu.VMEM((row_dev, 1, cols), jnp.float32),
            pltpu.VMEM((col_dev, 1, cols), jnp.float32),
            pltpu.VMEM((row_dev, 1, cols), jnp.float32),
            pltpu.VMEM((row_dev, 1, cols), jnp.float32),
            pltpu.VMEM((2, 1, cols), jnp.float32),
            pltpu.VMEM((2, 8, cols), jnp.float32),
            pltpu.VMEM((rows, cols), jnp.bfloat16),
            dma((11,)), dma((9,)),
            dma((3, chunks)), dma((7,)), dma((2, chunks)), dma((4,)), dma((chunks + 3,)),
            pltpu.SemaphoreType.REGULAR((2,)),
        ],
        compiler_params=pltpu.CompilerParams(
            collective_id=0, has_side_effects=True,
            vmem_limit_bytes=63 * 2**20 - 2 * rows * cols,
        ),
    )(values, tile_mask.T, keep_mask.T, thr_index.reshape(1, cols))


def on_device(values, tile_mask, keep_mask, thr_index, *, row_dev, col_dev):
    rows, cols = values.shape
    width = max(w for w in range(1, row_dev + 1) if row_dev % w == 0 and w * w <= row_dev)
    chips = col_dev // CORES
    if chips == 4 and row_dev == 4 and rows == CORES * cols:
        return near_call(
            values, tile_mask, keep_mask, thr_index, row_dev=row_dev, col_dev=col_dev, width=width
        )
    dma = pltpu.SemaphoreType.DMA
    vmem = pl.BlockSpec(memory_space=pltpu.VMEM)
    pruned, scale = pl.pallas_call(
        functools.partial(kernel, row_dev, col_dev, width, CHUNKS, rows * row_dev),
        out_shape=(
            pltpu.VMEM((rows, cols), jnp.float32),
            jax.ShapeDtypeStruct((1, cols), jnp.float32),
        ),
        in_specs=[pl.BlockSpec(memory_space=pl.ANY)] + [vmem] * 3,
        out_specs=(vmem, vmem),
        scratch_shapes=[
            pltpu.VMEM((col_dev, rows, cols), jnp.bfloat16),
            pltpu.VMEM((row_dev * rows, cols), jnp.bfloat16),
            pltpu.VMEM((row_dev, 1, cols), jnp.float32),
            pltpu.VMEM((col_dev, 1, cols), jnp.float32),
            dma((2, chips, CHUNKS)),
            dma((chips, CHUNKS)),
            dma((chips, CHUNKS)),
            dma((chips, CHUNKS)),
            dma((2, row_dev, CHUNKS)),
            dma((row_dev, CHUNKS)),
            dma((row_dev,)),
            dma((row_dev,)),
            dma((col_dev,)),
            dma((col_dev,)),
            pltpu.VMEM((rows, cols), jnp.bfloat16),
            dma((CHUNKS,)),
            pltpu.SemaphoreType.REGULAR((2,)),
        ],
        compiler_params=pltpu.CompilerParams(
            collective_id=0, has_side_effects=True,
            vmem_limit_bytes=63 * 2**20 - 4 * rows * cols + 2**19,
        ),
    )(values, tile_mask.T, keep_mask.T, thr_index.reshape(1, cols))
    return (pruned * scale).astype(jnp.bfloat16)


def solution(mesh):
    return jax.shard_map(
        functools.partial(on_device, row_dev=mesh.shape["row"], col_dev=mesh.shape["col"]),
        mesh=mesh,
        in_specs=(P("row", "col"), P("row", "col"), P("row", "col"), P("col")),
        out_specs=P("row", "col"),
        check_vma=False,
    )
```

```python
import functools

import jax
import jax.numpy as jnp
from jax import lax
from jax.experimental import pallas as pl
from jax.experimental.pallas import tpu as pltpu
from jax.sharding import PartitionSpec as P

TB = 128
CORES = 2
CHUNKS = 4


def snake(index, width):
    line, spot = index // width, index % width
    return line * width + spot + (line % 2) * (width - 1 - 2 * spot)


def kernel(
    row_dev, col_dev, width, chunks, order,
    v_ref, tile_ref, keep_ref, thr_ref, acc, totals_ref,
    row_panel, col_panel, sums, stats,
    line_send, line_recv, pair_send, pair_recv, ring_send, ring_recv,
    sum_send, sum_recv, stat_send, stat_recv, loaded, load_sem, token,
):
    rows, cols = v_ref.shape
    step_rows = rows // chunks
    chips = col_dev // CORES
    half = row_dev // 2
    me_row, me_col = lax.axis_index("row"), lax.axis_index("col")
    z, core = me_col // CORES, me_col % CORES
    pos = snake(me_row, width)

    def ring_device(offset):
        return snake((pos + offset + row_dev) % row_dev, width)

    barrier = pltpu.get_barrier_semaphore()
    pl.semaphore_signal(barrier, inc=1, device_id={"col": z * CORES + 1 - core})
    peers = 1 + (z > 0).astype(jnp.int32) + (z < chips - 1).astype(jnp.int32)
    for offset in ((1, -1) if row_dev > 2 else (1,) * half):
        pl.semaphore_signal(barrier, inc=1, device_id={"row": ring_device(offset)})
        peers += 1

    @pl.when(z > 0)
    def _():
        pl.semaphore_signal(barrier, inc=1, device_id={"col": me_col - CORES})

    @pl.when(z < chips - 1)
    def _():
        pl.semaphore_signal(barrier, inc=1, device_id={"col": me_col + CORES})

    def load(q):
        spot = pl.ds(q * step_rows, step_rows)
        return pltpu.make_async_copy(v_ref.at[spot], loaded.at[spot], load_sem.at[q])

    for q in range(chunks):
        load(q).start()

    stored = tile_ref[...].astype(jnp.float32)
    kept = keep_ref[...].astype(jnp.float32)
    height = min(step_rows, TB)
    for lo in range(0, rows, height):
        if lo % step_rows == 0:
            load(lo // step_rows).wait()
        for b in range(cols // TB):
            r, c = slice(lo, lo + height), slice(b * TB, (b + 1) * TB)
            scale = jnp.broadcast_to(stored[b : b + 1, lo // TB : lo // TB + 1], (height, TB))
            tile = (loaded[r, c].astype(jnp.float32) * scale).astype(jnp.bfloat16)
            row_panel[me_col, r, c] = tile
            col_panel[pl.ds(pl.multiple_of(me_row * rows + lo, height), height), c] = tile

    pl.semaphore_wait(barrier, peers)

    def row_part(block, q):
        return row_panel.at[block, pl.ds(q * step_rows, step_rows)]

    def line_copy(zi, q, to_right):
        part = row_part(zi * CORES + core, q)
        return pltpu.make_async_remote_copy(
            src_ref=part, dst_ref=part,
            send_sem=line_send.at[to_right, zi, q], recv_sem=line_recv.at[zi, q],
            device_id={"col": me_col + (CORES if to_right else -CORES)},
        )

    def pair_copy(zi, q, lane):
        part = row_part(zi * CORES + lane, q)
        return pltpu.make_async_remote_copy(
            src_ref=part, dst_ref=part,
            send_sem=pair_send.at[zi, q], recv_sem=pair_recv.at[zi, q],
            device_id={"col": z * CORES + 1 - core},
        )

    def ring_copy(owner, q, to_right):
        start = pl.multiple_of(owner * rows + q * step_rows, step_rows)
        part = col_panel.at[pl.ds(start, step_rows)]
        return pltpu.make_async_remote_copy(
            src_ref=part, dst_ref=part,
            send_sem=ring_send.at[to_right, owner, q], recv_sem=ring_recv.at[owner, q],
            device_id={"row": ring_device(1 if to_right else -1)},
        )

    def on_ring(d, q, to_right):
        if d < half:
            return True
        return d == half and (q < chunks // 2) == bool(to_right)

    def relay(zi, q, to_right, wait):
        if wait:
            line_copy(zi, q, to_right).wait_recv()
        go = (z < chips - 1) if to_right else (z > 0)

        @pl.when(go)
        def _():
            line_copy(zi, q, to_right).start()

    for q in range(chunks):
        for to_right in (1, 0):
            relay(z, q, to_right, False)
            if on_ring(1, q, to_right):
                ring_copy(me_row, q, to_right).start()
        pair_copy(z, q, core).start()

    for to_right in (1, 0):
        first, end = (0, chips - 1) if to_right else (chips - 1, 0)

        @pl.when(z != first)
        def _():
            pl.semaphore_wait(token.at[to_right], 1)

        @pl.when(z != end)
        def _():
            pl.semaphore_signal(
                token.at[to_right], inc=1,
                device_id={"col": me_col + (CORES if to_right else -CORES)},
            )

    def line_step(t, q):
        for to_right in (1, 0):
            valid = (z >= t) if to_right else (z + t < chips)
            zi = z - t if to_right else z + t
            if t < chips:
                @pl.when(valid)
                def _():
                    relay(zi, q, to_right, True)
                    pair_copy(zi, q, core).start()

    def ring_step(t, q):
        for to_right in (1, 0):
            if on_ring(t, q, to_right):
                owner = ring_device(-t if to_right else t)
                ring_copy(owner, q, to_right).wait_recv()
                if on_ring(t + 1, q, to_right):
                    ring_copy(owner, q, to_right).start()

    def stat_copy(d):
        return pltpu.make_async_remote_copy(
            src_ref=stats.at[0], dst_ref=stats.at[d],
            send_sem=stat_send.at[d], recv_sem=stat_recv.at[d],
            device_id={"col": (me_col + d) % col_dev},
        )

    def send_stats():
        total = jnp.zeros((1, cols), jnp.float32)
        for i in range(row_dev):
            block = col_panel[i * rows : (i + 1) * rows].astype(jnp.float32)
            total += jnp.sum(block, axis=0, keepdims=True)
        stats[0] = total
        for d in range(1, col_dev):
            stat_copy(d).start()

    def product_sums():
        total = jnp.zeros((1, cols), jnp.float32)
        for d in range(col_dev):
            if d:
                stat_copy(d).wait()
            block = (me_col - d + col_dev) % col_dev
            inner = pl.ds(pl.multiple_of(block * cols, cols), cols)
            rest, terms = stats[d], []
            for _ in range(3):
                term = rest.astype(jnp.bfloat16).astype(jnp.float32)
                rest = rest - term
                terms.append(jnp.broadcast_to(term, (8, cols)))
            spread = jnp.dot(
                jnp.concatenate(terms, axis=0).astype(jnp.bfloat16), col_panel[inner],
                preferred_element_type=jnp.float32,
            )
            total += spread[16:17] + spread[8:9] + spread[0:1]
        return total

    def compute(zi, q, first=False):
        spot = pl.ds(pl.multiple_of(q * step_rows, step_rows), step_rows)
        total = None
        for lane in range(CORES):
            block = zi * CORES + lane
            inner = pl.ds(pl.multiple_of(block * cols, cols), cols)
            term = jnp.dot(
                row_panel[block, spot], col_panel[inner], preferred_element_type=jnp.float32
            )
            total = term if total is None else total + term
        if first:
            acc[spot] = total
        else:
            acc[spot] += total

    def take(zi, q, first=False):
        pair_copy(zi, q, 1 - core).wait_recv()
        compute(zi, q, first)

    def sides(t):
        return ((z >= t, z - t), (z + t < chips, z + t))

    def bulk(upto):
        @pl.loop(0, chunks)
        def _(q):
            take(z, q, True)
            for t in range(1, min(upto, chips - 1) + 1):
                for valid, zi in sides(t):
                    @pl.when(valid)
                    def _():
                        take(zi, q)

    def prune(q, cut):
        parts = []
        for b in range(cols // TB):
            c = slice(b * TB, (b + 1) * TB)
            part = jnp.zeros((1, TB), jnp.float32)
            for lo in range(q * step_rows, (q + 1) * step_rows, min(step_rows, TB)):
                r = slice(lo, lo + min(step_rows, TB))
                keep = jnp.broadcast_to(kept[b : b + 1, lo // TB : lo // TB + 1], (r.stop - lo, TB))
                pruned = jnp.maximum(acc[r, c] - cut[:, c], 0.0) * keep
                acc[r, c] = pruned
                part += jnp.sum(pruned, axis=0, keepdims=True)
            parts.append(part)
        return jnp.concatenate(parts, axis=1)

    def cuts():
        return 0.125 * thr_ref[...].astype(jnp.float32) * (product_sums() / order)

    part = jnp.zeros((1, cols), jnp.float32)
    last = max(chips - 1, half)
    if half == 0:
        send_stats()
        bulk(0)
    for t in range(1, last + 1):
        if t == half:
            for q in range(chunks):
                ring_step(t, q)
            send_stats()
            for q in range(chunks):
                line_step(t, q)
            bulk(t)
        else:
            if t == last and t > half:
                cut = cuts()
            for q in range(chunks):
                line_step(t, q)
                if t < half:
                    ring_step(t, q)
                else:
                    for valid, zi in sides(t):
                        @pl.when(valid)
                        def _():
                            take(zi, q)
                    if t == last:
                        part += prune(q, cut)
    if last <= half:
        cut = cuts()
        for q in range(chunks):
            part += prune(q, cut)

    sums[0] = part

    def sum_copy(d):
        return pltpu.make_async_remote_copy(
            src_ref=sums.at[0], dst_ref=sums.at[d],
            send_sem=sum_send.at[d], recv_sem=sum_recv.at[d],
            device_id={"row": (me_row + d) % row_dev},
        )

    for d in range(1, row_dev):
        sum_copy(d).start()
    for d in range(1, row_dev):
        sum_copy(d).wait()
        part += sums[d]
    totals_ref[...] = 1.0 / jnp.maximum(part / order, 0.1)

    for q in range(chunks):
        for zi in range(chips):
            pair_copy(zi, q, core).wait_send()

            @pl.when((z < chips - 1) & (z >= zi))
            def _():
                line_copy(zi, q, 1).wait_send()

            @pl.when((z > 0) & (z <= zi))
            def _():
                line_copy(zi, q, 0).wait_send()
        for d in range(0, half):
            for to_right in (1, 0):
                if on_ring(d + 1, q, to_right):
                    owner = ring_device(-d if to_right else d)
                    ring_copy(owner, q, to_right).wait_send()


def cut_rows(lo, hi):
    while lo < hi:
        stop = min(hi, (lo // TB + 1) * TB)
        yield lo, stop
        lo = stop


def near_kernel(
    width, bounds, split, order,
    v_ref, tile_hbm, keep_hbm, thr_hbm, out_ref, acc, tile_ref, keep_ref, thr_ref,
    row_panel, col_panel, far, done, ahead, detour,
    row_sums, stats, sums, raw_sums, ahead_sums, total_sums, notes, loaded,
    sent, small, line_recv, pair_recv, ring_recv, far_recv, load_sem, token,
):
    rows, cols = v_ref.shape
    row_dev, col_dev, chips = row_sums.shape[0], stats.shape[0], stats.shape[0] // CORES
    chunks = len(bounds) - 1
    ahead_of = chunks - 1
    base = bounds[ahead_of]
    raw = range(ahead_of)
    me_row, me_col = lax.axis_index("row"), lax.axis_index("col")
    z, core = me_col // CORES, me_col % CORES
    pos = snake(me_row, width)
    on_right = z >= chips // 2
    end = jnp.where(on_right, chips - 1, 0)
    out = jnp.where(on_right, 1, -1)
    near, over, other = end - out, end - 2 * out, end - 3 * out
    is_end = z == end
    is_near = z == near
    inward, outward = me_col - CORES * out, me_col + CORES * out

    def ring_device(offset):
        return snake((pos + offset + row_dev) % row_dev, width)

    opposite = ring_device(2)

    barrier = pltpu.get_barrier_semaphore()
    for d in range(1, row_dev):
        pl.semaphore_signal(barrier, inc=1, device_id={"row": (me_row + d) % row_dev})
    pl.semaphore_signal(barrier, inc=1, device_id={"col": z * CORES + 1 - core})
    pl.semaphore_signal(barrier, inc=1, device_id={"col": inward})

    @pl.when(is_near)
    def _():
        pl.semaphore_signal(barrier, inc=1, device_id={"col": outward})


    def span(q):
        return pl.ds(bounds[q], bounds[q + 1] - bounds[q])

    def block_rows(owner, q):
        return pl.ds(pl.multiple_of(owner * rows + bounds[q], 16), bounds[q + 1] - bounds[q])

    def load(q):
        return pltpu.make_async_copy(v_ref.at[span(q)], loaded.at[span(q)], load_sem.at[q])

    def remote(src, dst, send, recv, device):
        return pltpu.make_async_remote_copy(
            src_ref=src, dst_ref=dst, send_sem=send, recv_sem=recv, device_id=device
        )

    def drain(ref, sem):
        pltpu.make_async_copy(ref, ref, sem).wait()

    def line(zi, kind, q, to_end):
        part = row_panel.at[zi * CORES + core, span(q)]
        return remote(
            part, part, sent.at[to_end], line_recv.at[kind, q],
            {"col": outward if to_end else inward},
        )

    def pair(zi, q, slot):
        part = row_panel.at[zi * CORES + core, span(q)]
        return remote(
            part, part, sent.at[2], pair_recv.at[slot], {"col": z * CORES + 1 - core}
        )

    def ring(owner, q, to_right, last):
        part = col_panel.at[block_rows(owner, q)]
        return remote(
            part, part, sent.at[3], ring_recv.at[last, q],
            {"row": ring_device(1 if to_right else -1)},
        )

    def far_ring(q, to_right):
        return remote(
            row_panel.at[end * CORES + core, span(q)], far.at[block_rows(me_row, q)],
            sent.at[4], far_recv.at[q // 2], {"row": ring_device(1 if to_right else -1)},
        )

    def far_own(q):
        return pltpu.make_async_copy(
            row_panel.at[end * CORES + core, span(q)], far.at[block_rows(me_row, q)], small.at[7]
        )

    def far_line(q):
        part = block_rows(opposite, q)
        return remote(
            col_panel.at[part], far.at[part], sent.at[1], far_recv.at[2 + q // 2], {"col": inward}
        )

    def detour_cross():
        return remote(
            row_panel.at[near * CORES + core, span(0)], detour, sent.at[4], small.at[8],
            {"row": opposite},
        )

    def detour_down():
        return remote(
            detour, col_panel.at[block_rows(opposite, 0)], sent.at[10], ring_recv.at[1, 0],
            {"col": inward},
        )

    def row_sum_copy(d):
        return remote(
            row_sums.at[0], row_sums.at[d], sent.at[5], small.at[0],
            {"row": (me_row + d) % row_dev},
        )

    def stat_copy(d):
        return remote(
            stats.at[0], stats.at[d], sent.at[6], small.at[1], {"col": (me_col + d) % col_dev}
        )

    def sum_copy(d):
        return remote(
            sums.at[0], sums.at[d], sent.at[7], small.at[2], {"row": (me_row + d) % row_dev}
        )

    def raw_sum_copy(d):
        return remote(
            sums.at[0], raw_sums.at[d], sent.at[11], small.at[9],
            {"row": (me_row + d) % row_dev, "col": inward},
        )

    def ahead_sum_copy(d):
        return remote(
            total_sums.at[0], ahead_sums.at[d], sent.at[8], small.at[3],
            {"row": (me_row + d) % row_dev, "col": outward},
        )

    def beside_sum_copy(d):
        return remote(
            total_sums.at[0], total_sums.at[d], sent.at[12], small.at[10],
            {"row": (me_row + d) % row_dev},
        )

    def note_copy():
        return remote(notes.at[0], notes.at[1], sent.at[9], small.at[4], {"col": inward})

    def early_copy():
        return remote(
            ahead.at[pl.ds(0, split)], acc.at[pl.ds(base, split)],
            sent.at[9], small.at[5], {"col": outward},
        )

    def done_copy():
        return remote(
            done, out_ref.at[pl.ds(base + split, rows - base - split)],
            sent.at[10], small.at[6], {"col": outward},
        )

    def own_ring(q):
        for to_right in (1, 0):
            ring(me_row, q, to_right, 0).start()

    def ring_wait(q):
        drain(col_panel.at[pl.ds(0, 2 * (bounds[q + 1] - bounds[q]))], ring_recv.at[0, q])

    def ring_relay_both(q):
        middle = (bounds[q] + bounds[q + 1]) // 32 * 16
        for to_right in (1, 0):
            lo, hi = (bounds[q], middle) if to_right else (middle, bounds[q + 1])
            owner = ring_device(-1 if to_right else 1)
            part = col_panel.at[pl.ds(pl.multiple_of(owner * rows + lo, 16), hi - lo)]
            remote(
                part, part, sent.at[3], ring_recv.at[1, q],
                {"row": ring_device(1 if to_right else -1)},
            ).start()

    def ring_relay(q, to_right):
        ring(ring_device(-1 if to_right else 1), q, to_right, 1).start()

    def ring_last(q):
        drain(col_panel.at[pl.ds(0, bounds[q + 1] - bounds[q])], ring_recv.at[1, q])

    def pair_slot(at_end, kind, q):
        if at_end:
            return 0 if kind == 0 else 2 * q + kind
        return 0 if q in raw else 1 + (kind == 2)

    def first_sends(q):
        @pl.when(is_end)
        def _():
            line(end, 0, q, 0).start()
            if q in (0, ahead_of):
                own_ring(q)
            if q in raw:
                pair(end, q, pair_slot(True, 0, q)).start()

        @pl.when(is_near)
        def _():
            if q < 2:
                line(near, 1, q, 0).start()
                own_ring(q)
            if q in raw:
                line(near, 0, q, 1).start()
            pair(near, q, pair_slot(False, 0, q)).start()

    tables = [
        pltpu.make_async_copy(src, dst, load_sem.at[chunks + i])
        for i, (src, dst) in enumerate(
            ((tile_hbm, tile_ref), (keep_hbm, keep_ref), (thr_hbm, thr_ref))
        )
    ]
    load(0).start()
    for table in tables:
        table.start()
    for q in range(1, chunks):
        load(q).start()
    for table in tables:
        table.wait()

    stored = tile_ref[...].astype(jnp.float32)
    kept = keep_ref[...].astype(jnp.float32)
    tile_sums = [jnp.zeros((1, TB), jnp.float32) for _ in range(cols // TB)]

    def mask(q):
        load(q).wait()
        for lo, hi in cut_rows(bounds[q], bounds[q + 1]):
            for b in range(cols // TB):
                r, c = slice(lo, hi), slice(b * TB, (b + 1) * TB)
                scale = jnp.broadcast_to(stored[b : b + 1, lo // TB : lo // TB + 1], (hi - lo, TB))
                tile = loaded[r, c].astype(jnp.float32) * scale
                tile_sums[b] += jnp.sum(tile, axis=0, keepdims=True)
                tile = tile.astype(jnp.bfloat16)
                row_panel[me_col, r, c] = tile
                col_panel[pl.ds(pl.multiple_of(me_row * rows + lo, 16), hi - lo), c] = tile

    mask(0)
    mask(1)
    pl.semaphore_wait(barrier, row_dev + 1 + is_near.astype(jnp.int32))

    @pl.when(is_end)
    def _():
        pl.semaphore_signal(token.at[0], inc=1, device_id={"col": inward})

    first_sends(0)
    mask(2)
    first_sends(1)
    mask(3)
    row_sums[0] = jnp.concatenate(tile_sums, axis=1)
    first_sends(2)
    for d in range(1, row_dev):
        row_sum_copy(d).start()
    first_sends(3)

    def send_stats():
        drain(row_sums.at[pl.ds(1, row_dev - 1)], small.at[0])
        total = row_sums[0]
        for d in range(1, row_dev):
            total += row_sums[d]
        stats[0] = total
        for d in range(1, col_dev):
            stat_copy(d).start()

    def wait_stats():
        drain(stats.at[pl.ds(1, col_dev - 1)], small.at[1])

    def inner(owner, lane):
        return pl.ds(pl.multiple_of((owner * CORES + lane) * cols, cols), cols)

    def product_sums(owners, lanes=range(CORES)):
        total = jnp.zeros((1, cols), jnp.float32)
        for owner in owners:
            for lane in lanes:
                rest = stats[(me_col - owner * CORES - lane + col_dev) % col_dev]
                terms = []
                for _ in range(3):
                    term = rest.astype(jnp.bfloat16).astype(jnp.float32)
                    rest = rest - term
                    terms.append(jnp.broadcast_to(term, (8, cols)))
                spread = jnp.dot(
                    jnp.concatenate(terms, axis=0).astype(jnp.bfloat16),
                    col_panel[inner(owner, lane)], preferred_element_type=jnp.float32,
                )
                total += spread[16:17] + spread[8:9] + spread[0:1]
        return total

    def cuts(total):
        return 0.125 * thr_ref[...].astype(jnp.float32) * (total / order)

    def product(zis, q, lanes=range(CORES), panel=col_panel):
        total = None
        for zi in zis:
            for lane in lanes:
                term = jnp.dot(
                    row_panel[zi * CORES + lane, span(q)], panel[inner(zi, lane)],
                    preferred_element_type=jnp.float32,
                )
                total = term if total is None else total + term
        return total

    def prune(q, cut):
        parts = []
        for b in range(cols // TB):
            c = slice(b * TB, (b + 1) * TB)
            part = jnp.zeros((1, TB), jnp.float32)
            for lo, hi in cut_rows(bounds[q], bounds[q + 1]):
                keep = jnp.broadcast_to(kept[b : b + 1, lo // TB : lo // TB + 1], (hi - lo, TB))
                pruned = jnp.maximum(acc[lo:hi, c] - cut[:, c], 0.0) * keep
                acc[lo:hi, c] = pruned
                part += jnp.sum(pruned, axis=0, keepdims=True)
            parts.append(part)
        return jnp.concatenate(parts, axis=1)

    def normal(total):
        return 1.0 / jnp.maximum(total / order, 0.1)

    def all_sums():
        drain(sums.at[pl.ds(1, row_dev - 1)], small.at[2])
        part = sums[0]
        for d in range(1, row_dev):
            part += sums[d]
        return part

    @pl.when(is_end)
    def _():
        def arrive(kind, q):
            zi = (near, over, other)[kind]
            drain(row_panel.at[0, span(q)], line_recv.at[kind, q])
            pair(zi, q, pair_slot(True, kind, q)).start()

        def met(kind, q):
            drain(row_panel.at[0, span(q)], pair_recv.at[pair_slot(True, kind, q)])

        ring_wait(0)
        ring_relay(0, 1)
        own_ring(1)
        arrive(0, 0)
        arrive(0, 1)
        ring_wait(3)
        ring_relay(3, 0)
        own_ring(2)
        arrive(0, 2)
        ring_last(0)
        far_line(0).start()
        pl.semaphore_wait(token.at[1], 1)
        send_stats()
        arrive(1, 0)
        ring_wait(1)
        ring_relay(1, 1)
        ring_last(3)
        far_line(3).start()
        arrive(1, 1)
        ring_wait(2)
        ring_relay(2, 0)
        detour_cross().start()
        ring_last(1)
        far_line(1).start()
        arrive(2, 0)
        ring_last(2)
        far_line(2).start()
        wait_stats()
        cut = cuts(product_sums(range(chips)))
        note = [cut]
        for t in range(base // TB, base // TB + 7):
            t = min(t, rows // TB - 1)
            line_of = [
                jnp.broadcast_to(kept[b : b + 1, t : t + 1], (1, TB)) for b in range(cols // TB)
            ]
            note.append(jnp.concatenate(line_of, axis=1))
        notes[0] = jnp.concatenate(note, axis=0)
        drain(row_panel.at[pl.ds(0, 2), pl.ds(0, base)], pair_recv.at[0])
        acc[span(2)] = product((end, near), 2)
        note_copy().start()
        met(1, 0)
        met(1, 1)
        acc[span(1)] = product((end, near, over), 1)
        met(2, 0)
        acc[span(0)] = product((end, near, over, other), 0)
        part = prune(0, cut)
        drain(detour, small.at[8])
        detour_down().start()
        arrive(1, 2)
        arrive(2, 1)
        met(1, 2)
        acc[span(2)] += product((over,), 2)
        met(2, 1)
        acc[span(1)] += product((other,), 1)
        part += prune(1, cut)
        arrive(2, 2)
        met(2, 2)
        acc[span(2)] += product((other,), 2)
        part += prune(2, cut)
        sums[0] = part
        for d in range(row_dev):
            raw_sum_copy(d).start()
        for d in range(1, row_dev):
            sum_copy(d).start()
        drain(ahead_sums, small.at[3])
        part = all_sums()
        for d in range(row_dev):
            part += ahead_sums[d]
        scale = normal(part)
        out_ref[:base] = (acc[:base] * scale).astype(jnp.bfloat16)
        drain(ahead.at[pl.ds(0, split)], small.at[5])
        out_ref[base : base + split] = (acc[base : base + split] * scale).astype(jnp.bfloat16)
        drain(done, small.at[6])
        drain(row_panel.at[0], sent.at[0])
        drain(col_panel.at[pl.ds(0, rows)], sent.at[1])
        drain(row_panel.at[pl.ds(0, chips), pl.ds(0, base)], sent.at[2])
        drain(notes.at[0], sent.at[9])
        drain(raw_sums, sent.at[11])
        drain(col_panel.at[pl.ds(0, 3 * rows)], sent.at[3])
        drain(detour, sent.at[4])
        drain(detour, sent.at[10])

    @pl.when(is_near)
    def _():
        def arrive(kind, q, relay):
            zi = (end, over, other)[kind]
            drain(row_panel.at[0, span(q)], line_recv.at[kind, q])
            if relay is not None:
                line(zi, 2 if kind == 0 else kind, q, relay).start()
            pair(zi, q, pair_slot(False, kind, q)).start()

        def from_end(q):
            arrive(0, q, 0)
            if q % 2 == 0:
                line(near, 1, 2 + q // 2, 0).start()
            for to_right in (1, 0):
                far_ring(q, to_right).start()
            far_own(q).start()
            if q < 2:
                own_ring(q + 2)

        def from_over(kind, q):
            arrive(kind, q, 1 if q in raw else None)

        beside = (me_row, ring_device(1), ring_device(-1))
        from_end(0)
        pl.semaphore_wait(token.at[0], 1)
        pl.semaphore_signal(token.at[1], inc=1, device_id={"col": inward})
        from_over(1, 0)
        from_end(1)
        from_over(1, 1)
        pl.semaphore_wait(token.at[1], 1)
        pl.semaphore_signal(token.at[1], inc=1, device_id={"col": outward})
        send_stats()
        from_end(2)
        from_over(2, 0)
        from_end(3)
        ring_wait(0)
        ring_wait(1)
        ring_relay(1, 1)
        from_over(1, 2)
        ring_wait(2)
        from_over(2, 1)
        ring_wait(3)
        ring_relay(3, 0)
        from_over(2, 2)
        drain(row_panel.at[pl.ds(0, chips), pl.ds(0, base)], pair_recv.at[0])
        for q in raw:
            acc[span(q)] = product(beside, q)
        from_over(1, 3)
        drain(row_panel.at[pl.ds(0, 3), span(ahead_of)], pair_recv.at[1])
        drain(far.at[pl.ds(0, rows)], small.at[7])
        drain(far.at[pl.ds(0, 2 * bounds[2])], far_recv.at[0])
        drain(far.at[pl.ds(0, bounds[2])], far_recv.at[2])
        ahead[...] = product((end, near, over), ahead_of, (0,), far)
        from_over(2, 3)
        drain(far.at[pl.ds(0, 2 * (rows - bounds[2]))], far_recv.at[1])
        drain(far.at[pl.ds(0, rows - bounds[2])], far_recv.at[3])
        ahead[...] += product((end, near, over), ahead_of, (1,), far)
        drain(row_panel.at[0, span(ahead_of)], pair_recv.at[2])
        ahead[...] += product((other,), ahead_of, range(CORES), far)
        drain(notes.at[1], small.at[4])
        parts = jnp.zeros((1, cols), jnp.float32)
        for lo, hi in cut_rows(base, rows):
            tile = lo // TB - base // TB + 1
            pruned = jnp.maximum(ahead[lo - base : hi - base] - notes[1, 0:1], 0.0)
            pruned *= notes[1, tile : tile + 1]
            ahead[lo - base : hi - base] = pruned
            parts += jnp.sum(pruned, axis=0, keepdims=True)
        total_sums[0] = parts
        for d in range(1, row_dev):
            beside_sum_copy(d).start()
        ring_relay_both(2)
        for d in range(row_dev):
            ahead_sum_copy(d).start()
        early_copy().start()
        acc[span(ahead_of)] = product(beside, ahead_of)
        wait_stats()
        head = product_sums(beside)
        ring_last(1)
        ring_last(0)
        for q in range(chunks):
            acc[span(q)] += product((opposite,), q, (0,))
        head += product_sums((opposite,), (0,))
        drain(total_sums.at[pl.ds(1, row_dev - 1)], small.at[10])
        drain(raw_sums, small.at[9])
        part = total_sums[0] + raw_sums[0]
        for d in range(1, row_dev):
            part += total_sums[d] + raw_sums[d]
        scale = normal(part)
        done[...] = (ahead[split:] * scale).astype(jnp.bfloat16)
        done_copy().start()
        ring_last(2)
        ring_last(3)
        cut = cuts(head + product_sums((opposite,), (1,)))
        part = jnp.zeros((1, cols), jnp.float32)
        for q in range(chunks):
            acc[span(q)] += product((opposite,), q, (1,))
            part += prune(q, cut)
        sums[0] = part
        for d in range(1, row_dev):
            sum_copy(d).start()
        out_ref[...] = (acc[...] * normal(all_sums())).astype(jnp.bfloat16)
        drain(row_panel.at[pl.ds(0, 2)], sent.at[0])
        drain(row_panel.at[pl.ds(0, 3), pl.ds(0, base)], sent.at[1])
        drain(row_panel.at[pl.ds(0, chips)], sent.at[2])
        drain(far.at[pl.ds(0, 2 * rows)], sent.at[4])
        drain(ahead_sums, sent.at[8])
        drain(total_sums.at[pl.ds(1, row_dev - 1)], sent.at[12])
        drain(ahead.at[pl.ds(0, split)], sent.at[9])
        drain(done, sent.at[10])
        drain(col_panel.at[pl.ds(0, 3 * rows - bounds[1])], sent.at[3])

    drain(row_sums.at[pl.ds(1, row_dev - 1)], sent.at[5])
    drain(stats.at[pl.ds(1, col_dev - 1)], sent.at[6])
    drain(sums.at[pl.ds(1, row_dev - 1)], sent.at[7])


def near_call(values, tile_mask, keep_mask, thr_index, *, row_dev, col_dev, width):
    rows, cols = values.shape
    base = rows * 45 // 64 // 16 * 16
    split = (rows - base) * 3 // 8 // 16 * 16
    bounds = (0, cols // 32 * 16, cols, base, rows)
    chunks = len(bounds) - 1
    dma = pltpu.SemaphoreType.DMA
    vmem = pl.BlockSpec(memory_space=pltpu.VMEM)
    return pl.pallas_call(
        functools.partial(near_kernel, width, bounds, split, rows * row_dev),
        out_shape=pltpu.VMEM((rows, cols), jnp.bfloat16),
        in_specs=[pl.BlockSpec(memory_space=pl.ANY)] * 4,
        out_specs=vmem,
        scratch_shapes=[
            pltpu.VMEM((rows, cols), jnp.float32),
            pltpu.VMEM(tile_mask.shape[::-1], jnp.int32),
            pltpu.VMEM(keep_mask.shape[::-1], jnp.int32),
            pltpu.VMEM((1, cols), jnp.int32),
            pltpu.VMEM((col_dev, rows, cols), jnp.bfloat16),
            pltpu.VMEM((row_dev * rows, cols), jnp.bfloat16),
            pltpu.VMEM((row_dev * rows, cols), jnp.bfloat16),
            pltpu.VMEM((rows - base - split, cols), jnp.bfloat16),
            pltpu.VMEM((rows - base, cols), jnp.float32),
            pltpu.VMEM((bounds[1], cols), jnp.bfloat16),
            pltpu.VMEM((row_dev, 1, cols), jnp.float32),
            pltpu.VMEM((col_dev, 1, cols), jnp.float32),
            pltpu.VMEM((row_dev, 1, cols), jnp.float32),
            pltpu.VMEM((row_dev, 1, cols), jnp.float32),
            pltpu.VMEM((row_dev, 1, cols), jnp.float32),
            pltpu.VMEM((row_dev, 1, cols), jnp.float32),
            pltpu.VMEM((2, 8, cols), jnp.float32),
            pltpu.VMEM((rows, cols), jnp.bfloat16),
            dma((13,)), dma((11,)),
            dma((3, chunks)), dma((7,)), dma((2, chunks)), dma((4,)), dma((chunks + 3,)),
            pltpu.SemaphoreType.REGULAR((2,)),
        ],
        compiler_params=pltpu.CompilerParams(
            collective_id=0, has_side_effects=True,
            vmem_limit_bytes=63 * 2**20 - 2 * rows * cols,
        ),
    )(values, tile_mask.T, keep_mask.T, thr_index.reshape(1, cols))


def on_device(values, tile_mask, keep_mask, thr_index, *, row_dev, col_dev):
    rows, cols = values.shape
    width = max(w for w in range(1, row_dev + 1) if row_dev % w == 0 and w * w <= row_dev)
    chips = col_dev // CORES
    if chips == 4 and row_dev == 4 and rows == CORES * cols:
        return near_call(
            values, tile_mask, keep_mask, thr_index, row_dev=row_dev, col_dev=col_dev, width=width
        )
    dma = pltpu.SemaphoreType.DMA
    vmem = pl.BlockSpec(memory_space=pltpu.VMEM)
    pruned, scale = pl.pallas_call(
        functools.partial(kernel, row_dev, col_dev, width, CHUNKS, rows * row_dev),
        out_shape=(
            pltpu.VMEM((rows, cols), jnp.float32),
            jax.ShapeDtypeStruct((1, cols), jnp.float32),
        ),
        in_specs=[pl.BlockSpec(memory_space=pl.ANY)] + [vmem] * 3,
        out_specs=(vmem, vmem),
        scratch_shapes=[
            pltpu.VMEM((col_dev, rows, cols), jnp.bfloat16),
            pltpu.VMEM((row_dev * rows, cols), jnp.bfloat16),
            pltpu.VMEM((row_dev, 1, cols), jnp.float32),
            pltpu.VMEM((col_dev, 1, cols), jnp.float32),
            dma((2, chips, CHUNKS)),
            dma((chips, CHUNKS)),
            dma((chips, CHUNKS)),
            dma((chips, CHUNKS)),
            dma((2, row_dev, CHUNKS)),
            dma((row_dev, CHUNKS)),
            dma((row_dev,)),
            dma((row_dev,)),
            dma((col_dev,)),
            dma((col_dev,)),
            pltpu.VMEM((rows, cols), jnp.bfloat16),
            dma((CHUNKS,)),
            pltpu.SemaphoreType.REGULAR((2,)),
        ],
        compiler_params=pltpu.CompilerParams(
            collective_id=0, has_side_effects=True,
            vmem_limit_bytes=63 * 2**20 - 4 * rows * cols + 2**19,
        ),
    )(values, tile_mask.T, keep_mask.T, thr_index.reshape(1, cols))
    return (pruned * scale).astype(jnp.bfloat16)


def solution(mesh):
    return jax.shard_map(
        functools.partial(on_device, row_dev=mesh.shape["row"], col_dev=mesh.shape["col"]),
        mesh=mesh,
        in_specs=(P("row", "col"), P("row", "col"), P("row", "col"), P("col")),
        out_specs=P("row", "col"),
        check_vma=False,
    )
```

```python
import functools

import jax
import jax.numpy as jnp
from jax import lax
from jax.experimental import pallas as pl
from jax.experimental.pallas import tpu as pltpu
from jax.sharding import PartitionSpec as P

TB = 128
CORES = 2
CHUNKS = 4


def snake(index, width):
    line, spot = index // width, index % width
    return line * width + spot + (line % 2) * (width - 1 - 2 * spot)


def kernel(
    row_dev, col_dev, width, chunks, order,
    v_ref, tile_ref, keep_ref, thr_ref, acc, totals_ref,
    row_panel, col_panel, sums, stats,
    line_send, line_recv, pair_send, pair_recv, ring_send, ring_recv,
    sum_send, sum_recv, stat_send, stat_recv, loaded, load_sem, token,
):
    rows, cols = v_ref.shape
    step_rows = rows // chunks
    chips = col_dev // CORES
    half = row_dev // 2
    me_row, me_col = lax.axis_index("row"), lax.axis_index("col")
    z, core = me_col // CORES, me_col % CORES
    pos = snake(me_row, width)

    def ring_device(offset):
        return snake((pos + offset + row_dev) % row_dev, width)

    barrier = pltpu.get_barrier_semaphore()
    pl.semaphore_signal(barrier, inc=1, device_id={"col": z * CORES + 1 - core})
    peers = 1 + (z > 0).astype(jnp.int32) + (z < chips - 1).astype(jnp.int32)
    for offset in ((1, -1) if row_dev > 2 else (1,) * half):
        pl.semaphore_signal(barrier, inc=1, device_id={"row": ring_device(offset)})
        peers += 1

    @pl.when(z > 0)
    def _():
        pl.semaphore_signal(barrier, inc=1, device_id={"col": me_col - CORES})

    @pl.when(z < chips - 1)
    def _():
        pl.semaphore_signal(barrier, inc=1, device_id={"col": me_col + CORES})

    def load(q):
        spot = pl.ds(q * step_rows, step_rows)
        return pltpu.make_async_copy(v_ref.at[spot], loaded.at[spot], load_sem.at[q])

    for q in range(chunks):
        load(q).start()

    stored = tile_ref[...].astype(jnp.float32)
    kept = keep_ref[...].astype(jnp.float32)
    height = min(step_rows, TB)
    for lo in range(0, rows, height):
        if lo % step_rows == 0:
            load(lo // step_rows).wait()
        for b in range(cols // TB):
            r, c = slice(lo, lo + height), slice(b * TB, (b + 1) * TB)
            scale = jnp.broadcast_to(stored[b : b + 1, lo // TB : lo // TB + 1], (height, TB))
            tile = (loaded[r, c].astype(jnp.float32) * scale).astype(jnp.bfloat16)
            row_panel[me_col, r, c] = tile
            col_panel[pl.ds(pl.multiple_of(me_row * rows + lo, height), height), c] = tile

    pl.semaphore_wait(barrier, peers)

    def row_part(block, q):
        return row_panel.at[block, pl.ds(q * step_rows, step_rows)]

    def line_copy(zi, q, to_right):
        part = row_part(zi * CORES + core, q)
        return pltpu.make_async_remote_copy(
            src_ref=part, dst_ref=part,
            send_sem=line_send.at[to_right, zi, q], recv_sem=line_recv.at[zi, q],
            device_id={"col": me_col + (CORES if to_right else -CORES)},
        )

    def pair_copy(zi, q, lane):
        part = row_part(zi * CORES + lane, q)
        return pltpu.make_async_remote_copy(
            src_ref=part, dst_ref=part,
            send_sem=pair_send.at[zi, q], recv_sem=pair_recv.at[zi, q],
            device_id={"col": z * CORES + 1 - core},
        )

    def ring_copy(owner, q, to_right):
        start = pl.multiple_of(owner * rows + q * step_rows, step_rows)
        part = col_panel.at[pl.ds(start, step_rows)]
        return pltpu.make_async_remote_copy(
            src_ref=part, dst_ref=part,
            send_sem=ring_send.at[to_right, owner, q], recv_sem=ring_recv.at[owner, q],
            device_id={"row": ring_device(1 if to_right else -1)},
        )

    def on_ring(d, q, to_right):
        if d < half:
            return True
        return d == half and (q < chunks // 2) == bool(to_right)

    def relay(zi, q, to_right, wait):
        if wait:
            line_copy(zi, q, to_right).wait_recv()
        go = (z < chips - 1) if to_right else (z > 0)

        @pl.when(go)
        def _():
            line_copy(zi, q, to_right).start()

    for q in range(chunks):
        for to_right in (1, 0):
            relay(z, q, to_right, False)
            if on_ring(1, q, to_right):
                ring_copy(me_row, q, to_right).start()
        pair_copy(z, q, core).start()

    for to_right in (1, 0):
        first, end = (0, chips - 1) if to_right else (chips - 1, 0)

        @pl.when(z != first)
        def _():
            pl.semaphore_wait(token.at[to_right], 1)

        @pl.when(z != end)
        def _():
            pl.semaphore_signal(
                token.at[to_right], inc=1,
                device_id={"col": me_col + (CORES if to_right else -CORES)},
            )

    def line_step(t, q):
        for to_right in (1, 0):
            valid = (z >= t) if to_right else (z + t < chips)
            zi = z - t if to_right else z + t
            if t < chips:
                @pl.when(valid)
                def _():
                    relay(zi, q, to_right, True)
                    pair_copy(zi, q, core).start()

    def ring_step(t, q):
        for to_right in (1, 0):
            if on_ring(t, q, to_right):
                owner = ring_device(-t if to_right else t)
                ring_copy(owner, q, to_right).wait_recv()
                if on_ring(t + 1, q, to_right):
                    ring_copy(owner, q, to_right).start()

    def stat_copy(d):
        return pltpu.make_async_remote_copy(
            src_ref=stats.at[0], dst_ref=stats.at[d],
            send_sem=stat_send.at[d], recv_sem=stat_recv.at[d],
            device_id={"col": (me_col + d) % col_dev},
        )

    def send_stats():
        total = jnp.zeros((1, cols), jnp.float32)
        for i in range(row_dev):
            block = col_panel[i * rows : (i + 1) * rows].astype(jnp.float32)
            total += jnp.sum(block, axis=0, keepdims=True)
        stats[0] = total
        for d in range(1, col_dev):
            stat_copy(d).start()

    def product_sums():
        total = jnp.zeros((1, cols), jnp.float32)
        for d in range(col_dev):
            if d:
                stat_copy(d).wait()
            block = (me_col - d + col_dev) % col_dev
            inner = pl.ds(pl.multiple_of(block * cols, cols), cols)
            rest, terms = stats[d], []
            for _ in range(3):
                term = rest.astype(jnp.bfloat16).astype(jnp.float32)
                rest = rest - term
                terms.append(jnp.broadcast_to(term, (8, cols)))
            spread = jnp.dot(
                jnp.concatenate(terms, axis=0).astype(jnp.bfloat16), col_panel[inner],
                preferred_element_type=jnp.float32,
            )
            total += spread[16:17] + spread[8:9] + spread[0:1]
        return total

    def compute(zi, q, first=False):
        spot = pl.ds(pl.multiple_of(q * step_rows, step_rows), step_rows)
        total = None
        for lane in range(CORES):
            block = zi * CORES + lane
            inner = pl.ds(pl.multiple_of(block * cols, cols), cols)
            term = jnp.dot(
                row_panel[block, spot], col_panel[inner], preferred_element_type=jnp.float32
            )
            total = term if total is None else total + term
        if first:
            acc[spot] = total
        else:
            acc[spot] += total

    def take(zi, q, first=False):
        pair_copy(zi, q, 1 - core).wait_recv()
        compute(zi, q, first)

    def sides(t):
        return ((z >= t, z - t), (z + t < chips, z + t))

    def bulk(upto):
        @pl.loop(0, chunks)
        def _(q):
            take(z, q, True)
            for t in range(1, min(upto, chips - 1) + 1):
                for valid, zi in sides(t):
                    @pl.when(valid)
                    def _():
                        take(zi, q)

    def prune(q, cut):
        parts = []
        for b in range(cols // TB):
            c = slice(b * TB, (b + 1) * TB)
            part = jnp.zeros((1, TB), jnp.float32)
            for lo in range(q * step_rows, (q + 1) * step_rows, min(step_rows, TB)):
                r = slice(lo, lo + min(step_rows, TB))
                keep = jnp.broadcast_to(kept[b : b + 1, lo // TB : lo // TB + 1], (r.stop - lo, TB))
                pruned = jnp.maximum(acc[r, c] - cut[:, c], 0.0) * keep
                acc[r, c] = pruned
                part += jnp.sum(pruned, axis=0, keepdims=True)
            parts.append(part)
        return jnp.concatenate(parts, axis=1)

    def cuts():
        return 0.125 * thr_ref[...].astype(jnp.float32) * (product_sums() / order)

    part = jnp.zeros((1, cols), jnp.float32)
    last = max(chips - 1, half)
    if half == 0:
        send_stats()
        bulk(0)
    for t in range(1, last + 1):
        if t == half:
            for q in range(chunks):
                ring_step(t, q)
            send_stats()
            for q in range(chunks):
                line_step(t, q)
            bulk(t)
        else:
            if t == last and t > half:
                cut = cuts()
            for q in range(chunks):
                line_step(t, q)
                if t < half:
                    ring_step(t, q)
                else:
                    for valid, zi in sides(t):
                        @pl.when(valid)
                        def _():
                            take(zi, q)
                    if t == last:
                        part += prune(q, cut)
    if last <= half:
        cut = cuts()
        for q in range(chunks):
            part += prune(q, cut)

    sums[0] = part

    def sum_copy(d):
        return pltpu.make_async_remote_copy(
            src_ref=sums.at[0], dst_ref=sums.at[d],
            send_sem=sum_send.at[d], recv_sem=sum_recv.at[d],
            device_id={"row": (me_row + d) % row_dev},
        )

    for d in range(1, row_dev):
        sum_copy(d).start()
    for d in range(1, row_dev):
        sum_copy(d).wait()
        part += sums[d]
    totals_ref[...] = 1.0 / jnp.maximum(part / order, 0.1)

    for q in range(chunks):
        for zi in range(chips):
            pair_copy(zi, q, core).wait_send()

            @pl.when((z < chips - 1) & (z >= zi))
            def _():
                line_copy(zi, q, 1).wait_send()

            @pl.when((z > 0) & (z <= zi))
            def _():
                line_copy(zi, q, 0).wait_send()
        for d in range(0, half):
            for to_right in (1, 0):
                if on_ring(d + 1, q, to_right):
                    owner = ring_device(-d if to_right else d)
                    ring_copy(owner, q, to_right).wait_send()


def cut_rows(lo, hi):
    while lo < hi:
        stop = min(hi, (lo // TB + 1) * TB)
        yield lo, stop
        lo = stop


def near_kernel(
    width, bounds, splits, order,
    v_ref, tile_hbm, keep_hbm, thr_hbm, out_ref, acc, tile_ref, keep_ref, thr_ref,
    row_panel, col_panel, far, done, ahead, detour,
    row_sums, stats, sums, raw_sums, ahead_sums, total_sums, notes, loaded,
    sent, small, line_recv, pair_recv, ring_recv, far_recv, load_sem, token,
):
    rows, cols = v_ref.shape
    row_dev, col_dev, chips = row_sums.shape[0], stats.shape[0], stats.shape[0] // CORES
    chunks = len(bounds) - 1
    ahead_of = chunks - 1
    base = bounds[ahead_of]
    raw = range(ahead_of)
    me_row, me_col = lax.axis_index("row"), lax.axis_index("col")
    z, core = me_col // CORES, me_col % CORES
    pos = snake(me_row, width)
    on_right = z >= chips // 2
    end = jnp.where(on_right, chips - 1, 0)
    out = jnp.where(on_right, 1, -1)
    near, over, other = end - out, end - 2 * out, end - 3 * out
    is_end = z == end
    is_near = z == near
    inward, outward = me_col - CORES * out, me_col + CORES * out

    def ring_device(offset):
        return snake((pos + offset + row_dev) % row_dev, width)

    opposite = ring_device(2)

    barrier = pltpu.get_barrier_semaphore()
    for d in range(1, row_dev):
        pl.semaphore_signal(barrier, inc=1, device_id={"row": (me_row + d) % row_dev})
    pl.semaphore_signal(barrier, inc=1, device_id={"col": z * CORES + 1 - core})
    pl.semaphore_signal(barrier, inc=1, device_id={"col": inward})

    @pl.when(is_near)
    def _():
        pl.semaphore_signal(barrier, inc=1, device_id={"col": outward})


    def span(q):
        return pl.ds(bounds[q], bounds[q + 1] - bounds[q])

    def block_rows(owner, q):
        return pl.ds(pl.multiple_of(owner * rows + bounds[q], 16), bounds[q + 1] - bounds[q])

    def load(q):
        return pltpu.make_async_copy(v_ref.at[span(q)], loaded.at[span(q)], load_sem.at[q])

    def remote(src, dst, send, recv, device):
        return pltpu.make_async_remote_copy(
            src_ref=src, dst_ref=dst, send_sem=send, recv_sem=recv, device_id=device
        )

    def drain(ref, sem):
        pltpu.make_async_copy(ref, ref, sem).wait()

    def line(zi, kind, q, to_end):
        part = row_panel.at[zi * CORES + core, span(q)]
        return remote(
            part, part, sent.at[to_end], line_recv.at[kind, q],
            {"col": outward if to_end else inward},
        )

    def pair(zi, q, slot):
        part = row_panel.at[zi * CORES + core, span(q)]
        return remote(
            part, part, sent.at[2], pair_recv.at[slot], {"col": z * CORES + 1 - core}
        )

    def ring(owner, q, to_right, last):
        part = col_panel.at[block_rows(owner, q)]
        return remote(
            part, part, sent.at[3], ring_recv.at[last, q],
            {"row": ring_device(1 if to_right else -1)},
        )

    def far_ring(q, to_right):
        return remote(
            row_panel.at[end * CORES + core, span(q)], far.at[block_rows(me_row, q)],
            sent.at[4], far_recv.at[q // 2], {"row": ring_device(1 if to_right else -1)},
        )

    def far_own(q):
        return pltpu.make_async_copy(
            row_panel.at[end * CORES + core, span(q)], far.at[block_rows(me_row, q)], small.at[7]
        )

    def far_line(q):
        part = block_rows(opposite, q)
        return remote(
            col_panel.at[part], far.at[part], sent.at[1], far_recv.at[2 + q // 2], {"col": inward}
        )

    def detour_cross():
        return remote(
            row_panel.at[near * CORES + core, span(0)], detour, sent.at[4], small.at[8],
            {"row": opposite},
        )

    def detour_down():
        return remote(
            detour, col_panel.at[block_rows(opposite, 0)], sent.at[10], ring_recv.at[1, 0],
            {"col": inward},
        )

    def row_sum_copy(d):
        return remote(
            row_sums.at[0], row_sums.at[d], sent.at[5], small.at[0],
            {"row": (me_row + d) % row_dev},
        )

    def stat_copy(d):
        return remote(
            stats.at[0], stats.at[d], sent.at[6], small.at[1], {"col": (me_col + d) % col_dev}
        )

    def sum_copy(d):
        return remote(
            sums.at[0], sums.at[d], sent.at[7], small.at[2], {"row": (me_row + d) % row_dev}
        )

    def raw_sum_copy(d):
        return remote(
            sums.at[0], raw_sums.at[d], sent.at[11], small.at[9],
            {"row": (me_row + d) % row_dev, "col": inward},
        )

    def ahead_sum_copy(d):
        return remote(
            total_sums.at[0], ahead_sums.at[d], sent.at[8], small.at[3],
            {"row": (me_row + d) % row_dev, "col": outward},
        )

    def beside_sum_copy(d):
        return remote(
            total_sums.at[0], total_sums.at[d], sent.at[12], small.at[10],
            {"row": (me_row + d) % row_dev},
        )

    def note_copy():
        return remote(notes.at[0], notes.at[1], sent.at[9], small.at[4], {"col": inward})

    def early_copy(c):
        return remote(
            ahead.at[pl.ds(0, splits[c])], acc.at[pl.ds(base, splits[c])],
            sent.at[9], small.at[5], {"col": outward},
        )

    def done_copy(c):
        return remote(
            done.at[pl.ds(splits[c], rows - base - splits[c])],
            out_ref.at[pl.ds(base + splits[c], rows - base - splits[c])],
            sent.at[10], small.at[6], {"col": outward},
        )

    def on_core(act):
        for c in range(CORES):
            pl.when(core == c)(functools.partial(act, c))

    def own_ring(q):
        for to_right in (1, 0):
            ring(me_row, q, to_right, 0).start()

    def ring_wait(q):
        drain(col_panel.at[pl.ds(0, 2 * (bounds[q + 1] - bounds[q]))], ring_recv.at[0, q])

    def ring_relay_both(q):
        middle = (bounds[q] + bounds[q + 1]) // 32 * 16
        for to_right in (1, 0):
            lo, hi = (bounds[q], middle) if to_right else (middle, bounds[q + 1])
            owner = ring_device(-1 if to_right else 1)
            part = col_panel.at[pl.ds(pl.multiple_of(owner * rows + lo, 16), hi - lo)]
            remote(
                part, part, sent.at[3], ring_recv.at[1, q],
                {"row": ring_device(1 if to_right else -1)},
            ).start()

    def ring_relay(q, to_right):
        ring(ring_device(-1 if to_right else 1), q, to_right, 1).start()

    def ring_last(q):
        drain(col_panel.at[pl.ds(0, bounds[q + 1] - bounds[q])], ring_recv.at[1, q])

    def pair_slot(at_end, kind, q):
        if at_end:
            return 0 if kind == 0 else 2 * q + kind
        return 0 if q in raw else 1 + (kind == 2)

    def first_sends(q):
        @pl.when(is_end)
        def _():
            line(end, 0, q, 0).start()
            if q in (0, ahead_of):
                own_ring(q)
            if q in raw:
                pair(end, q, pair_slot(True, 0, q)).start()

        @pl.when(is_near)
        def _():
            if q < 2:
                line(near, 1, q, 0).start()
                own_ring(q)
            if q in raw:
                line(near, 0, q, 1).start()
            pair(near, q, pair_slot(False, 0, q)).start()

    tables = [
        pltpu.make_async_copy(src, dst, load_sem.at[chunks + i])
        for i, (src, dst) in enumerate(
            ((tile_hbm, tile_ref), (keep_hbm, keep_ref), (thr_hbm, thr_ref))
        )
    ]
    load(0).start()
    for table in tables:
        table.start()
    for q in range(1, chunks):
        load(q).start()
    for table in tables:
        table.wait()

    stored = tile_ref[...].astype(jnp.float32)
    kept = keep_ref[...].astype(jnp.float32)
    tile_sums = [jnp.zeros((1, TB), jnp.float32) for _ in range(cols // TB)]

    def mask(q):
        load(q).wait()
        for lo, hi in cut_rows(bounds[q], bounds[q + 1]):
            for b in range(cols // TB):
                r, c = slice(lo, hi), slice(b * TB, (b + 1) * TB)
                scale = jnp.broadcast_to(stored[b : b + 1, lo // TB : lo // TB + 1], (hi - lo, TB))
                tile = loaded[r, c].astype(jnp.float32) * scale
                tile_sums[b] += jnp.sum(tile, axis=0, keepdims=True)
                tile = tile.astype(jnp.bfloat16)
                row_panel[me_col, r, c] = tile
                col_panel[pl.ds(pl.multiple_of(me_row * rows + lo, 16), hi - lo), c] = tile

    mask(0)
    mask(1)
    pl.semaphore_wait(barrier, row_dev + 1 + is_near.astype(jnp.int32))

    @pl.when(is_end)
    def _():
        pl.semaphore_signal(token.at[0], inc=1, device_id={"col": inward})

    first_sends(0)
    mask(2)
    first_sends(1)
    mask(3)
    row_sums[0] = jnp.concatenate(tile_sums, axis=1)
    first_sends(2)
    for d in range(1, row_dev):
        row_sum_copy(d).start()
    first_sends(3)

    def send_stats():
        drain(row_sums.at[pl.ds(1, row_dev - 1)], small.at[0])
        total = row_sums[0]
        for d in range(1, row_dev):
            total += row_sums[d]
        stats[0] = total
        for d in range(1, col_dev):
            stat_copy(d).start()

    def wait_stats():
        drain(stats.at[pl.ds(1, col_dev - 1)], small.at[1])

    def inner(owner, lane):
        return pl.ds(pl.multiple_of((owner * CORES + lane) * cols, cols), cols)

    def product_sums(owners, lanes=range(CORES)):
        total = jnp.zeros((1, cols), jnp.float32)
        for owner in owners:
            for lane in lanes:
                rest = stats[(me_col - owner * CORES - lane + col_dev) % col_dev]
                terms = []
                for _ in range(3):
                    term = rest.astype(jnp.bfloat16).astype(jnp.float32)
                    rest = rest - term
                    terms.append(jnp.broadcast_to(term, (8, cols)))
                spread = jnp.dot(
                    jnp.concatenate(terms, axis=0).astype(jnp.bfloat16),
                    col_panel[inner(owner, lane)], preferred_element_type=jnp.float32,
                )
                total += spread[16:17] + spread[8:9] + spread[0:1]
        return total

    def cuts(total):
        return 0.125 * thr_ref[...].astype(jnp.float32) * (total / order)

    def product(zis, q, lanes=range(CORES), panel=col_panel):
        total = None
        for zi in zis:
            for lane in lanes:
                term = jnp.dot(
                    row_panel[zi * CORES + lane, span(q)], panel[inner(zi, lane)],
                    preferred_element_type=jnp.float32,
                )
                total = term if total is None else total + term
        return total

    def prune(q, cut):
        parts = []
        for b in range(cols // TB):
            c = slice(b * TB, (b + 1) * TB)
            part = jnp.zeros((1, TB), jnp.float32)
            for lo, hi in cut_rows(bounds[q], bounds[q + 1]):
                keep = jnp.broadcast_to(kept[b : b + 1, lo // TB : lo // TB + 1], (hi - lo, TB))
                pruned = jnp.maximum(acc[lo:hi, c] - cut[:, c], 0.0) * keep
                acc[lo:hi, c] = pruned
                part += jnp.sum(pruned, axis=0, keepdims=True)
            parts.append(part)
        return jnp.concatenate(parts, axis=1)

    def normal(total):
        return 1.0 / jnp.maximum(total / order, 0.1)

    def all_sums():
        drain(sums.at[pl.ds(1, row_dev - 1)], small.at[2])
        part = sums[0]
        for d in range(1, row_dev):
            part += sums[d]
        return part

    @pl.when(is_end)
    def _():
        def arrive(kind, q):
            zi = (near, over, other)[kind]
            drain(row_panel.at[0, span(q)], line_recv.at[kind, q])
            pair(zi, q, pair_slot(True, kind, q)).start()

        def met(kind, q):
            drain(row_panel.at[0, span(q)], pair_recv.at[pair_slot(True, kind, q)])

        ring_wait(0)
        ring_relay(0, 1)
        own_ring(1)
        arrive(0, 0)
        arrive(0, 1)
        ring_wait(3)
        ring_relay(3, 0)
        own_ring(2)
        arrive(0, 2)
        ring_last(0)
        far_line(0).start()
        pl.semaphore_wait(token.at[1], 1)
        send_stats()
        arrive(1, 0)
        ring_wait(1)
        ring_relay(1, 1)
        ring_last(3)
        far_line(3).start()
        arrive(1, 1)
        ring_wait(2)
        ring_relay(2, 0)
        detour_cross().start()
        ring_last(1)
        far_line(1).start()
        arrive(2, 0)
        ring_last(2)
        far_line(2).start()
        wait_stats()
        cut = cuts(product_sums(range(chips)))
        note = [cut]
        for t in range(base // TB, base // TB + 7):
            t = min(t, rows // TB - 1)
            line_of = [
                jnp.broadcast_to(kept[b : b + 1, t : t + 1], (1, TB)) for b in range(cols // TB)
            ]
            note.append(jnp.concatenate(line_of, axis=1))
        notes[0] = jnp.concatenate(note, axis=0)
        drain(row_panel.at[pl.ds(0, 2), pl.ds(0, base)], pair_recv.at[0])
        acc[span(2)] = product((end, near), 2)
        note_copy().start()
        met(1, 0)
        met(1, 1)
        acc[span(1)] = product((end, near, over), 1)
        met(2, 0)
        acc[span(0)] = product((end, near, over, other), 0)
        part = prune(0, cut)
        drain(detour, small.at[8])
        detour_down().start()
        arrive(1, 2)
        arrive(2, 1)
        met(1, 2)
        acc[span(2)] += product((over,), 2)
        met(2, 1)
        acc[span(1)] += product((other,), 1)
        part += prune(1, cut)
        arrive(2, 2)
        met(2, 2)
        acc[span(2)] += product((other,), 2)
        part += prune(2, cut)
        sums[0] = part
        for d in range(row_dev):
            raw_sum_copy(d).start()
        for d in range(1, row_dev):
            sum_copy(d).start()
        drain(ahead_sums, small.at[3])
        part = all_sums()
        for d in range(row_dev):
            part += ahead_sums[d]
        scale = normal(part)
        out_ref[:base] = (acc[:base] * scale).astype(jnp.bfloat16)

        def finish(c):
            stop = base + splits[c]
            drain(ahead.at[pl.ds(0, splits[c])], small.at[5])
            out_ref[base:stop] = (acc[base:stop] * scale).astype(jnp.bfloat16)
            drain(done.at[pl.ds(splits[c], rows - stop)], small.at[6])

        on_core(finish)
        drain(row_panel.at[0], sent.at[0])
        drain(col_panel.at[pl.ds(0, rows)], sent.at[1])
        drain(row_panel.at[pl.ds(0, chips), pl.ds(0, base)], sent.at[2])
        drain(notes.at[0], sent.at[9])
        drain(raw_sums, sent.at[11])
        drain(col_panel.at[pl.ds(0, 3 * rows)], sent.at[3])
        drain(detour, sent.at[4])
        drain(detour, sent.at[10])

    @pl.when(is_near)
    def _():
        def arrive(kind, q, relay):
            zi = (end, over, other)[kind]
            drain(row_panel.at[0, span(q)], line_recv.at[kind, q])
            if relay is not None:
                line(zi, 2 if kind == 0 else kind, q, relay).start()
            pair(zi, q, pair_slot(False, kind, q)).start()

        def from_end(q):
            arrive(0, q, 0)
            if q % 2 == 0:
                line(near, 1, 2 + q // 2, 0).start()
            for to_right in (1, 0):
                far_ring(q, to_right).start()
            far_own(q).start()
            if q < 2:
                own_ring(q + 2)

        def from_over(kind, q):
            arrive(kind, q, 1 if q in raw else None)

        beside = (me_row, ring_device(1), ring_device(-1))
        from_end(0)
        pl.semaphore_wait(token.at[0], 1)
        pl.semaphore_signal(token.at[1], inc=1, device_id={"col": inward})
        from_over(1, 0)
        from_end(1)
        from_over(1, 1)
        pl.semaphore_wait(token.at[1], 1)
        pl.semaphore_signal(token.at[1], inc=1, device_id={"col": outward})
        send_stats()
        from_end(2)
        from_over(2, 0)
        from_end(3)
        ring_wait(0)
        ring_wait(1)
        ring_relay(1, 1)
        from_over(1, 2)
        ring_wait(2)
        from_over(2, 1)
        ring_wait(3)
        ring_relay(3, 0)
        from_over(2, 2)
        drain(row_panel.at[pl.ds(0, chips), pl.ds(0, base)], pair_recv.at[0])
        for q in raw:
            acc[span(q)] = product(beside, q)
        from_over(1, 3)
        drain(row_panel.at[pl.ds(0, 3), span(ahead_of)], pair_recv.at[1])
        drain(far.at[pl.ds(0, rows)], small.at[7])
        drain(far.at[pl.ds(0, 2 * bounds[2])], far_recv.at[0])
        drain(far.at[pl.ds(0, bounds[2])], far_recv.at[2])
        ahead[...] = product((end, near, over), ahead_of, (0,), far)
        drain(notes.at[1], small.at[4])
        drain(far.at[pl.ds(0, 2 * (rows - bounds[2]))], far_recv.at[1])
        drain(far.at[pl.ds(0, rows - bounds[2])], far_recv.at[3])
        ahead[...] += product((end, near, over), ahead_of, (1,), far)
        from_over(2, 3)
        ahead[...] += product((other,), ahead_of, (core,), far)
        drain(row_panel.at[0, span(ahead_of)], pair_recv.at[2])
        ahead[...] += product((other,), ahead_of, (1 - core,), far)
        parts = jnp.zeros((1, cols), jnp.float32)
        for lo, hi in cut_rows(base, rows):
            tile = lo // TB - base // TB + 1
            pruned = jnp.maximum(ahead[lo - base : hi - base] - notes[1, 0:1], 0.0)
            pruned *= notes[1, tile : tile + 1]
            ahead[lo - base : hi - base] = pruned
            parts += jnp.sum(pruned, axis=0, keepdims=True)
        total_sums[0] = parts
        for d in range(1, row_dev):
            beside_sum_copy(d).start()
        ring_relay_both(2)
        for d in range(row_dev):
            ahead_sum_copy(d).start()
        on_core(lambda c: early_copy(c).start())
        acc[span(ahead_of)] = product(beside, ahead_of)
        wait_stats()
        head = product_sums(beside)
        ring_last(1)
        ring_last(0)
        for q in range(chunks):
            acc[span(q)] += product((opposite,), q, (0,))
        head += product_sums((opposite,), (0,))
        drain(total_sums.at[pl.ds(1, row_dev - 1)], small.at[10])
        drain(raw_sums, small.at[9])
        part = total_sums[0] + raw_sums[0]
        for d in range(1, row_dev):
            part += total_sums[d] + raw_sums[d]
        scale = normal(part)
        first = min(splits)
        done[first:] = (ahead[first:] * scale).astype(jnp.bfloat16)
        on_core(lambda c: done_copy(c).start())
        ring_last(2)
        ring_last(3)
        cut = cuts(head + product_sums((opposite,), (1,)))
        part = jnp.zeros((1, cols), jnp.float32)
        for q in range(chunks):
            acc[span(q)] += product((opposite,), q, (1,))
            part += prune(q, cut)
        sums[0] = part
        for d in range(1, row_dev):
            sum_copy(d).start()
        out_ref[...] = (acc[...] * normal(all_sums())).astype(jnp.bfloat16)
        drain(row_panel.at[pl.ds(0, 2)], sent.at[0])
        drain(row_panel.at[pl.ds(0, 3), pl.ds(0, base)], sent.at[1])
        drain(row_panel.at[pl.ds(0, chips)], sent.at[2])
        drain(far.at[pl.ds(0, 2 * rows)], sent.at[4])
        drain(ahead_sums, sent.at[8])
        drain(total_sums.at[pl.ds(1, row_dev - 1)], sent.at[12])

        def drain_ahead(c):
            drain(ahead.at[pl.ds(0, splits[c])], sent.at[9])
            drain(done.at[pl.ds(splits[c], rows - base - splits[c])], sent.at[10])

        on_core(drain_ahead)
        drain(col_panel.at[pl.ds(0, 3 * rows - bounds[1])], sent.at[3])

    drain(row_sums.at[pl.ds(1, row_dev - 1)], sent.at[5])
    drain(stats.at[pl.ds(1, col_dev - 1)], sent.at[6])
    drain(sums.at[pl.ds(1, row_dev - 1)], sent.at[7])


def near_call(values, tile_mask, keep_mask, thr_index, *, row_dev, col_dev, width):
    rows, cols = values.shape
    base = rows * 45 // 64 // 16 * 16
    splits = tuple((rows - base) * n // 16 // 16 * 16 for n in (7, 3))
    bounds = (0, cols // 32 * 16, cols, base, rows)
    chunks = len(bounds) - 1
    dma = pltpu.SemaphoreType.DMA
    vmem = pl.BlockSpec(memory_space=pltpu.VMEM)
    return pl.pallas_call(
        functools.partial(near_kernel, width, bounds, splits, rows * row_dev),
        out_shape=pltpu.VMEM((rows, cols), jnp.bfloat16),
        in_specs=[pl.BlockSpec(memory_space=pl.ANY)] * 4,
        out_specs=vmem,
        scratch_shapes=[
            pltpu.VMEM((rows, cols), jnp.float32),
            pltpu.VMEM(tile_mask.shape[::-1], jnp.int32),
            pltpu.VMEM(keep_mask.shape[::-1], jnp.int32),
            pltpu.VMEM((1, cols), jnp.int32),
            pltpu.VMEM((col_dev, rows, cols), jnp.bfloat16),
            pltpu.VMEM((row_dev * rows, cols), jnp.bfloat16),
            pltpu.VMEM((row_dev * rows, cols), jnp.bfloat16),
            pltpu.VMEM((rows - base, cols), jnp.bfloat16),
            pltpu.VMEM((rows - base, cols), jnp.float32),
            pltpu.VMEM((bounds[1], cols), jnp.bfloat16),
            pltpu.VMEM((row_dev, 1, cols), jnp.float32),
            pltpu.VMEM((col_dev, 1, cols), jnp.float32),
            pltpu.VMEM((row_dev, 1, cols), jnp.float32),
            pltpu.VMEM((row_dev, 1, cols), jnp.float32),
            pltpu.VMEM((row_dev, 1, cols), jnp.float32),
            pltpu.VMEM((row_dev, 1, cols), jnp.float32),
            pltpu.VMEM((2, 8, cols), jnp.float32),
            pltpu.VMEM((rows, cols), jnp.bfloat16),
            dma((13,)), dma((11,)),
            dma((3, chunks)), dma((7,)), dma((2, chunks)), dma((4,)), dma((chunks + 3,)),
            pltpu.SemaphoreType.REGULAR((2,)),
        ],
        compiler_params=pltpu.CompilerParams(
            collective_id=0, has_side_effects=True,
            vmem_limit_bytes=63 * 2**20 - 2 * rows * cols,
        ),
    )(values, tile_mask.T, keep_mask.T, thr_index.reshape(1, cols))


def on_device(values, tile_mask, keep_mask, thr_index, *, row_dev, col_dev):
    rows, cols = values.shape
    width = max(w for w in range(1, row_dev + 1) if row_dev % w == 0 and w * w <= row_dev)
    chips = col_dev // CORES
    if chips == 4 and row_dev == 4 and rows == CORES * cols:
        return near_call(
            values, tile_mask, keep_mask, thr_index, row_dev=row_dev, col_dev=col_dev, width=width
        )
    dma = pltpu.SemaphoreType.DMA
    vmem = pl.BlockSpec(memory_space=pltpu.VMEM)
    pruned, scale = pl.pallas_call(
        functools.partial(kernel, row_dev, col_dev, width, CHUNKS, rows * row_dev),
        out_shape=(
            pltpu.VMEM((rows, cols), jnp.float32),
            jax.ShapeDtypeStruct((1, cols), jnp.float32),
        ),
        in_specs=[pl.BlockSpec(memory_space=pl.ANY)] + [vmem] * 3,
        out_specs=(vmem, vmem),
        scratch_shapes=[
            pltpu.VMEM((col_dev, rows, cols), jnp.bfloat16),
            pltpu.VMEM((row_dev * rows, cols), jnp.bfloat16),
            pltpu.VMEM((row_dev, 1, cols), jnp.float32),
            pltpu.VMEM((col_dev, 1, cols), jnp.float32),
            dma((2, chips, CHUNKS)),
            dma((chips, CHUNKS)),
            dma((chips, CHUNKS)),
            dma((chips, CHUNKS)),
            dma((2, row_dev, CHUNKS)),
            dma((row_dev, CHUNKS)),
            dma((row_dev,)),
            dma((row_dev,)),
            dma((col_dev,)),
            dma((col_dev,)),
            pltpu.VMEM((rows, cols), jnp.bfloat16),
            dma((CHUNKS,)),
            pltpu.SemaphoreType.REGULAR((2,)),
        ],
        compiler_params=pltpu.CompilerParams(
            collective_id=0, has_side_effects=True,
            vmem_limit_bytes=63 * 2**20 - 4 * rows * cols + 2**19,
        ),
    )(values, tile_mask.T, keep_mask.T, thr_index.reshape(1, cols))
    return (pruned * scale).astype(jnp.bfloat16)


def solution(mesh):
    return jax.shard_map(
        functools.partial(on_device, row_dev=mesh.shape["row"], col_dev=mesh.shape["col"]),
        mesh=mesh,
        in_specs=(P("row", "col"), P("row", "col"), P("row", "col"), P("col")),
        out_specs=P("row", "col"),
        check_vma=False,
    )
```
